32 devices in a mesh: arow: 4 (over z), acol: 8 (over y, x, core).
Axes of the slice: x: 2, y: 2, z: 4, core: 2. Of those that a mesh axis runs over, the one named last changes fastest.
Arguments:
- row_data: bfloat16 [65536, 128], P(('arow', 'acol')), may hold values from -96 to 96
- row_baseline: int32 [65536], P(('arow', 'acol')), may hold values from 0 to 131071, as said below
- pair_table: int32 [131072, 2], P(('arow', 'acol')), may hold values from 0 to 2047, as said below
- lengths: int32 [131072], P(('arow', 'acol')), may hold values from 1 to 8
- model_vis: bfloat16 [2048, 2048, 128], P('arow', 'acol'), may hold values from -6 to 6
- gains: float32 [2048, 128], P(('arow', 'acol')), may hold values from -6 to 6
Outputs:
- new_gains: float32 [2048, 128], P(('arow', 'acol'))
The draws below stay inside these ranges and needn't reach their ends.
Inputs may be any that keep to these rules, and one draw needn't show every extreme that they name: `pair_table`: slot j belongs to tile o = j // 4096; its first antenna lies in 512 * (o // 8) to 512 * (o // 8 + 1) - 1, its second in 256 * (o % 8) to 256 * (o % 8 + 1) - 1, and the two differ. `row_baseline`: the rows of one device name slots of one tile at most 256 times; one tile is named exactly 256 times by the rows of every device.
All inputs are finite; a program needn't handle non-finite values.
Results may differ from the reference program's by a relative error of at most 0.0003.
Values may be sent and summed in bfloat16 or wider, within the bound.
A program may use at most 128 MiB of HBM per device.

```python
import jax
import jax.numpy as jnp
from jax import lax

A = 2048
F = 64
ROWS_DEV = 2048
BPO = 4096
AR = 512
AC = 256
CAP = 256
ROWS = 65536
NBW = 131072
DEVICES = 32


def draw_pair_table(key, part):
    index = jnp.arange(NBW, dtype=jnp.int32)
    owner = index // BPO
    blocks = A // AC
    first = owner // blocks * AR + jax.random.randint(jax.random.fold_in(key, 11), (NBW,), 0, AR, dtype=jnp.int32)
    pick = jax.random.randint(jax.random.fold_in(key, 12), (NBW,), 0, AC, dtype=jnp.int32)
    second = owner % blocks * AC + pick
    second = jnp.where(second == first, owner % blocks * AC + (pick + 1) % AC, second)
    return jnp.stack([first, second], axis=1)


def draw_row_baseline(key, part):
    spots = jnp.arange(ROWS_DEV, dtype=jnp.int32)
    flips = jax.random.randint(jax.random.fold_in(key, 21), (DEVICES, ROWS_DEV), 0, 2, dtype=jnp.int32)
    rest = spots[None, :] - CAP
    ranking = jnp.where(spots[None, :] < CAP, 0, 1 + (rest % (DEVICES - 1) + flips) % (DEVICES - 1))
    streams = jax.random.split(jax.random.fold_in(key, 22), DEVICES)
    mixed = jax.vmap(lambda stream, row: row[jax.random.permutation(stream, ROWS_DEV)])(streams, ranking)
    chosen = jax.random.permutation(jax.random.fold_in(key, 23), DEVICES).astype(jnp.int32)
    owner = chosen[mixed]
    pick = jax.random.randint(jax.random.fold_in(key, 24), (DEVICES, ROWS_DEV), 0, BPO, dtype=jnp.int32)
    return (owner * BPO + pick).reshape(ROWS).astype(jnp.int32)


def set_ends(result, stream_key, low, high):
    longest = result.shape.index(max(result.shape))
    spots = []
    for shift in (0, 1):
        where = [jax.random.randint(jax.random.fold_in(stream_key, axis), (), 0, length) for axis, length in enumerate(result.shape)]
        where[longest] = (where[longest] + shift) % result.shape[longest]
        spots.append(tuple(where))
    return result.at[spots[0]].set(low).at[spots[1]].set(high)


def levels(stream_key, shape, cuts, smallest, high):
    gain = 1.0
    for axis_at, shards_of in cuts:
        heights = jax.random.uniform(jax.random.fold_in(jax.random.fold_in(stream_key, 6), axis_at), (shards_of,), jnp.float32, smallest / len(cuts), high / len(cuts))
        gain = gain * jnp.repeat(jnp.exp(heights), shape[axis_at] // shards_of).reshape((-1,) + (1,) * (len(shape) - 1 - axis_at))
    return gain


def noise(stream_key, extent, spread, bound, pieces=(), held_as=jnp.bfloat16):
    entries = jax.random.normal(stream_key, extent, jnp.float32) * spread
    if len(pieces) > 0:
        entries = levels(stream_key, extent, pieces, -0.22, 0.18) * entries
    return jnp.clip(entries, min=-bound, max=bound).astype(held_as)


def setup_inputs(seed: int = 0) -> dict:
    streams_of = jax.random.split(jax.random.key(seed), 7)
    return {
        "row_data": noise(streams_of[0], (ROWS, 2 * F), 16.0, 96.0, ((0, 32),)),
        "row_baseline": draw_row_baseline(jax.random.fold_in(streams_of[6], 71), 0),
        "pair_table": draw_pair_table(jax.random.fold_in(streams_of[6], 71), 0),
        "lengths": set_ends(jax.random.randint(streams_of[3], (NBW,), 1, 9), jax.random.fold_in(streams_of[3], 1), 1, 8).astype(jnp.int32),
        "model_vis": noise(streams_of[4], (A, A, 2 * F), 1.0, 6.0, ((0, 4), (1, 8))),
        "gains": noise(streams_of[5], (A, 2 * F), 1.0, 6.0, ((0, 32),), jnp.float32),
    }


def reference(row_data, row_baseline, pair_table, lengths, model_vis, gains):
    pairs = pair_table[row_baseline]
    first = pairs[:, 0]
    second = pairs[:, 1]
    weight = lengths[row_baseline].astype(jnp.float32)
    terms = weight[:, None] * row_data.astype(jnp.float32)
    nant = gains.shape[0]
    half = gains.shape[1] // 2
    band = nant // 8
    g_re = gains[None, :, :half]
    g_im = gains[None, :, half:]

    def block(index):
        start = index * band
        local = first - start
        inside = (local >= 0) & (local < band)
        spot = jnp.where(inside, local * nant + second, band * nant)
        sums = jnp.zeros((band * nant + 1, 2 * half), jnp.float32).at[spot].add(terms)
        sums = sums[:-1].reshape(band, nant, 2 * half)
        totals = jnp.zeros((band * nant + 1,), jnp.float32).at[spot].add(weight)
        totals = totals[:-1].reshape(band, nant)
        model = lax.dynamic_slice_in_dim(model_vis, start, band, 0)
        m_re = model[..., :half].astype(jnp.float32)
        m_im = model[..., half:].astype(jnp.float32)
        c_re = m_re * g_re + m_im * g_im
        c_im = m_re * g_im - m_im * g_re
        s_re = sums[..., :half]
        s_im = sums[..., half:]
        num = jnp.concatenate([jnp.sum(c_re * s_re - c_im * s_im, axis=1), jnp.sum(c_re * s_im + c_im * s_re, axis=1)], axis=1)
        den = jnp.sum(totals[:, :, None] * (c_re * c_re + c_im * c_im), axis=1)
        return num, den

    nums, dens = lax.map(block, jnp.arange(8, dtype=jnp.int32))
    num = nums.reshape(nant, 2 * half)
    den = dens.reshape(nant, half)
    return jnp.concatenate([num[:, :half] / (den + 1.0), num[:, half:] / (den + 1.0)], axis=1)
```

```python
import functools

import jax
import jax.numpy as jnp
from jax import lax
from jax.experimental import pallas as pl
from jax.experimental.pallas import tpu as pltpu
from jax.sharding import PartitionSpec as P

RIDGE = 1.0
LANES = 128
GROUP = 32
WEIGHT_BITS = 4
MESH = pl.DeviceIdType.MESH


def rows_at(ref, start, count):
    return ref[pl.ds(start, count), :]


def route_kernel(
    devices, capacity, slots, rows_ref, base_ref, out_ref, label_ref,
    wide, spread, target, local_id, empty, target_s, local_s, sems,
):
    blocks = base_ref.shape[0]
    count = rows_ref.shape[0]
    empty[...] = jnp.full(empty.shape, slots, jnp.int32)
    fill = pltpu.make_async_copy(empty, label_ref, sems.at[0])
    fill.start()
    order = lax.broadcasted_iota(jnp.int32, (LANES, LANES), 0)
    upper = (order < lax.broadcasted_iota(jnp.int32, (LANES, LANES), 1)).astype(jnp.bfloat16)
    tile = lax.broadcasted_iota(jnp.int32, (devices, LANES), 0)
    before = jnp.zeros((devices, 1), jnp.float32)
    for block in range(blocks):
        slot = base_ref[block : block + 1, :]
        owner = slot // slots
        hit = tile == owner
        hits = jnp.where(hit, 1.0, 0.0)
        within = jnp.dot(hits.astype(jnp.bfloat16), upper, preferred_element_type=jnp.float32)
        ranking = jnp.sum(jnp.where(hit, within + before, 0.0), axis=0, keepdims=True)
        before = before + jnp.sum(hits, axis=1, keepdims=True)
        target[block : block + 1, :] = owner * capacity + ranking.astype(jnp.int32)
        local_id[block : block + 1, :] = slot - owner * slots
    to_target = pltpu.make_async_copy(target, target_s, sems.at[1])
    to_target.start()
    to_local = pltpu.make_async_copy(local_id, local_s, sems.at[2])
    to_local.start()
    wide[...] = rows_ref[...].astype(jnp.float32)
    spread[...] = jnp.zeros_like(spread)
    to_target.wait()
    to_local.wait()
    fill.wait()

    def place_block(block, carry):
        def place(group, carry):
            first = group * GROUP
            spots = [target_s[block, first + k] for k in range(GROUP)]
            ids = [local_s[block, first + k] for k in range(GROUP)]
            held = [
                wide[pl.ds(block * LANES + first + k, 1), :] for k in range(GROUP)
            ]
            for k in range(GROUP):
                label_ref[spots[k]] = ids[k]
                spread[pl.ds(spots[k], 1), :] = held[k]
            return carry

        return lax.fori_loop(0, LANES // GROUP, place, carry)

    lax.fori_loop(0, count // LANES, place_block, 0)
    out_ref[...] = spread[...].astype(jnp.bfloat16)


def route(rows, baseline, devices, capacity, slots):
    count, width = rows.shape
    blocks = count // LANES
    total = devices * capacity
    return pl.pallas_call(
        functools.partial(route_kernel, devices, capacity, slots),
        out_shape=(
            jax.ShapeDtypeStruct((total, width), jnp.bfloat16),
            jax.ShapeDtypeStruct((total,), jnp.int32),
        ),
        in_specs=[pl.BlockSpec(memory_space=pltpu.VMEM)] * 2,
        out_specs=(
            pl.BlockSpec(memory_space=pltpu.VMEM),
            pl.BlockSpec(memory_space=pltpu.SMEM),
        ),
        scratch_shapes=[
            pltpu.VMEM((count, width), jnp.float32),
            pltpu.VMEM((total, width), jnp.float32),
            pltpu.VMEM((blocks, LANES), jnp.int32),
            pltpu.VMEM((blocks, LANES), jnp.int32),
            pltpu.VMEM((total,), jnp.int32),
            pltpu.SMEM((blocks, LANES), jnp.int32),
            pltpu.SMEM((blocks, LANES), jnp.int32),
            pltpu.SemaphoreType.DMA((3,)),
        ],
        name="route",
    )(rows, baseline.reshape(blocks, LANES))


def share_kernel(
    row_count, col_count, label_ref, gain_ref, name_ref, column_ref,
    send_sem, recv_sem, gain_send, gain_recv, local_sem,
):
    devices = row_count * col_count
    my_row = lax.axis_index("arow")
    my_col = lax.axis_index("acol")
    me = my_row * col_count + my_col
    barrier = pltpu.get_barrier_semaphore()

    def place(index):
        return (index // col_count, lax.rem(index, col_count))

    def greet(step, carry):
        pl.semaphore_signal(
            barrier, inc=1, device_id=place(lax.rem(me + step, devices)), device_id_type=MESH
        )
        return carry

    lax.fori_loop(1, devices, greet, 0)
    own = pltpu.make_async_copy(label_ref.at[me], name_ref.at[me], local_sem.at[0])
    own.start()
    pl.semaphore_wait(barrier, devices - 1)

    def label_copy(to, slot):
        return pltpu.make_async_remote_copy(
            src_ref=label_ref.at[to],
            dst_ref=name_ref.at[slot],
            send_sem=send_sem.at[to],
            recv_sem=recv_sem.at[slot],
            device_id=place(to),
            device_id_type=MESH,
        )

    def send(step, carry):
        label_copy(lax.rem(me + step, devices), me).start()
        return carry

    lax.fori_loop(1, devices, send, 0)
    column = me // row_count
    part = lax.rem(me, row_count)

    def gain_copy(row, col, slot):
        return pltpu.make_async_remote_copy(
            src_ref=gain_ref,
            dst_ref=column_ref.at[slot],
            send_sem=gain_send.at[row],
            recv_sem=gain_recv.at[slot],
            device_id=(row, col),
            device_id_type=MESH,
        )

    own_gain = pltpu.make_async_copy(gain_ref, column_ref.at[part], local_sem.at[1])
    for row in range(row_count):
        stays = jnp.logical_and(row == my_row, column == my_col)

        @pl.when(jnp.logical_not(stays))
        def _():
            gain_copy(row, column, part).start()

        @pl.when(stays)
        def _():
            own_gain.start()

    for row in range(row_count):
        stays = jnp.logical_and(row == my_row, column == my_col)

        @pl.when(jnp.logical_not(stays))
        def _():
            gain_copy(row, column, part).wait_send()

        @pl.when(stays)
        def _():
            own_gain.wait()

    for slot in range(row_count):
        source = my_col * row_count + slot

        @pl.when(source != me)
        def _():
            gain_copy(0, my_col, slot).wait_recv()

    def finish(step, carry):
        other = lax.rem(me + step, devices)
        label_copy(other, other).wait()
        return carry

    lax.fori_loop(1, devices, finish, 0)
    own.wait()


def share(labels, gains, row_count, col_count):
    devices = row_count * col_count
    return pl.pallas_call(
        functools.partial(share_kernel, row_count, col_count),
        out_shape=(
            jax.ShapeDtypeStruct(labels.shape, jnp.int32),
            jax.ShapeDtypeStruct((row_count,) + gains.shape, jnp.float32),
        ),
        in_specs=[pl.BlockSpec(memory_space=pltpu.VMEM)] * 2,
        out_specs=(pl.BlockSpec(memory_space=pltpu.VMEM),) * 2,
        scratch_shapes=[
            pltpu.SemaphoreType.DMA((devices,)),
            pltpu.SemaphoreType.DMA((devices,)),
            pltpu.SemaphoreType.DMA((row_count,)),
            pltpu.SemaphoreType.DMA((row_count,)),
            pltpu.SemaphoreType.DMA((2,)),
        ],
        compiler_params=pltpu.CompilerParams(collective_id=0, has_side_effects=True),
        name="share",
    )(labels, gains)


def gather_kernel(
    col_block, chunk, name_ref, table_ref, model_ref, gain_ref, c_ref, info_ref,
    model, pair_gain, gain_rows, picked, sem,
):
    total = c_ref.shape[0]
    width = c_ref.shape[1]
    half = width // 2
    load = pltpu.make_async_copy(model_ref, model, sem)
    load.start()
    shift = col_block.bit_length() + WEIGHT_BITS
    odd = lax.broadcasted_iota(jnp.int32, gain_ref.shape, 0) & 1
    pair_gain[pl.ds(0, col_block, stride=2), :] = jnp.where(odd == 0, gain_ref[...], 0.0)
    pair_gain[pl.ds(1, col_block, stride=2), :] = jnp.where(odd == 1, gain_ref[...], 0.0)

    def look(group, carry):
        first = group * GROUP
        names = [name_ref[first + k] for k in range(GROUP)]
        infos = [table_ref[name] for name in names]
        held = [pair_gain[pl.ds(info & (2 * col_block - 1), 2), :] for info in infos]
        for k in range(GROUP):
            info_ref[first + k] = infos[k]
            gain_rows[pl.ds(2 * (first + k), 2), :] = held[k]
        return carry

    lax.fori_loop(0, total // GROUP, look, 0)
    load.wait()

    def piece(number, carry):
        start = number * chunk

        def fetch(group, carry):
            first = group * GROUP
            infos = [info_ref[start + first + k] for k in range(GROUP)]
            held = [model[info >> shift].astype(jnp.float32) for info in infos]
            for k in range(GROUP):
                picked[pl.ds(2 * (first + k), 2), :] = held[k]
            return carry

        lax.fori_loop(0, chunk // GROUP, fetch, 0)
        at = pl.multiple_of(2 * start, 2 * chunk)
        m_even = picked[pl.ds(0, chunk, stride=2), :]
        m_odd = picked[pl.ds(1, chunk, stride=2), :]
        g_even = gain_rows[pl.ds(at, chunk, stride=2), :]
        g_odd = gain_rows[pl.ds(at + 1, chunk, stride=2), :]
        a = m_even * g_even + m_odd * g_odd
        b = m_even * pltpu.roll(g_even, half, 1) + m_odd * pltpu.roll(g_odd, half, 1)
        low = lax.broadcasted_iota(jnp.int32, (chunk, width), 1) < half
        c_ref[pl.ds(pl.multiple_of(start, chunk), chunk), :] = jnp.where(
            low, a + pltpu.roll(a, half, 1), pltpu.roll(b, half, 1) - b
        )
        return carry

    lax.fori_loop(0, total // chunk, piece, 0)


def gather(names, table, model_vis, column_gains):
    row_block, col_block, width = model_vis.shape
    pairs = row_block * col_block // 2
    total = names.shape[0]
    chunk = min(512, total)
    return pl.pallas_call(
        functools.partial(gather_kernel, col_block, chunk),
        out_shape=(
            jax.ShapeDtypeStruct((total, width), jnp.float32),
            jax.ShapeDtypeStruct((total,), jnp.int32),
        ),
        in_specs=[
            pl.BlockSpec(memory_space=pltpu.SMEM),
            pl.BlockSpec(memory_space=pltpu.SMEM),
            pl.BlockSpec(memory_space=pl.ANY),
            pl.BlockSpec(memory_space=pltpu.VMEM),
        ],
        out_specs=(
            pl.BlockSpec(memory_space=pltpu.VMEM),
            pl.BlockSpec(memory_space=pltpu.SMEM),
        ),
        scratch_shapes=[
            pltpu.VMEM((pairs, 2, width), jnp.bfloat16),
            pltpu.VMEM((2 * col_block, width), jnp.float32),
            pltpu.VMEM((2 * total, width), jnp.float32),
            pltpu.VMEM((2 * chunk, width), jnp.float32),
            pltpu.SemaphoreType.DMA,
        ],
        compiler_params=pltpu.CompilerParams(vmem_limit_bytes=56 << 20),
        cost_estimate=pl.CostEstimate(
            flops=1 << 20, bytes_accessed=model_vis.size * 2, transcendentals=0
        ),
        name="gather",
    )(names, table, model_vis.reshape(pairs, 2, width), column_gains)


def pick_rows(info, row_block, col_block):
    column_bits = col_block.bit_length()
    first = info >> (2 * column_bits + WEIGHT_BITS - 2)
    weight = ((info >> column_bits) & ((1 << WEIGHT_BITS) - 1)).astype(jnp.float32)
    spots = lax.broadcasted_iota(jnp.int32, (row_block, info.shape[1]), 0)
    return jnp.where(spots == first, weight, 0.0).astype(jnp.bfloat16)


def power_kernel(col_block, info_ref, c_ref, out_ref):
    row_block, width = out_ref.shape
    half = width // 2

    @pl.when(pl.program_id(0) == 0)
    def _():
        out_ref[...] = jnp.zeros_like(out_ref)

    c = c_ref[...]
    power = c * c
    power = power + pltpu.roll(power, half, 1)
    high = power.astype(jnp.bfloat16).astype(jnp.float32)
    low = lax.broadcasted_iota(jnp.int32, power.shape, 1) < half
    values = jnp.where(low, high, power - high).astype(jnp.bfloat16)
    sums = jnp.dot(
        pick_rows(info_ref[0], row_block, col_block), values, preferred_element_type=jnp.float32
    )
    out_ref[...] += sums + pltpu.roll(sums, half, 1)


def product_kernel(col_block, info_ref, c_ref, rows_ref, out_ref):
    row_block, width = out_ref.shape
    half = width // 2

    @pl.when(pl.program_id(0) == 0)
    def _():
        out_ref[...] = jnp.zeros_like(out_ref)

    c = c_ref[...]
    r = rows_ref[...].astype(jnp.float32)
    a = c * r
    b = c * pltpu.roll(r, half, 1)
    low = lax.broadcasted_iota(jnp.int32, c.shape, 1) < half
    product = jnp.where(low, a - pltpu.roll(a, half, 1), b + pltpu.roll(b, half, 1))
    high = product.astype(jnp.bfloat16)
    rest = (product - high.astype(jnp.float32)).astype(jnp.bfloat16)
    values = jnp.concatenate([high, rest], axis=1)
    sums = jnp.dot(
        pick_rows(info_ref[0], row_block, col_block), values, preferred_element_type=jnp.float32
    )
    out_ref[...] += sums[:, :width] + sums[:, width:]


def segment(kernel, name, info, arrays, row_block, col_block):
    total, width = arrays[0].shape
    chunk = min(1024, total)
    steps = total // chunk
    return pl.pallas_call(
        functools.partial(kernel, col_block),
        out_shape=jax.ShapeDtypeStruct((row_block, width), jnp.float32),
        grid=(steps,),
        in_specs=[pl.BlockSpec((1, 1, chunk), lambda i: (i, 0, 0))]
        + [pl.BlockSpec((chunk, width), lambda i: (i, 0))] * len(arrays),
        out_specs=pl.BlockSpec((row_block, width), lambda i: (0, 0)),
        cost_estimate=pl.CostEstimate(
            flops=2 * row_block * total * 2 * width,
            bytes_accessed=total * width * 4,
            transcendentals=0,
        ),
        name=name,
    )(info.reshape(steps, 1, chunk), *arrays)


def collect_kernel(
    count, num_ref, den_ref, out_ref, num_held, den_held, num_send, num_recv, den_send, den_recv
):
    me = lax.axis_index("acol")
    barrier = pltpu.get_barrier_semaphore()
    for step in range(1, count):
        pl.semaphore_signal(
            barrier,
            inc=1,
            device_id=(lax.axis_index("arow"), lax.rem(me + step, count)),
            device_id_type=MESH,
        )
    pl.semaphore_wait(barrier, count - 1)

    def copies(to, slot):
        return [
            pltpu.make_async_remote_copy(
                src_ref=part.at[to],
                dst_ref=held.at[slot],
                send_sem=send.at[to],
                recv_sem=recv.at[slot],
                device_id=(lax.axis_index("arow"), to),
                device_id_type=MESH,
            )
            for part, held, send, recv in (
                (den_ref, den_held, den_send, den_recv),
                (num_ref, num_held, num_send, num_recv),
            )
        ]

    for step in range(1, count):
        for copy in copies(lax.rem(me + step, count), me):
            copy.start()
    num = num_ref[me]
    den = den_ref[me]
    for step in range(1, count):
        other = lax.rem(me + step, count)
        for copy in copies(other, other):
            copy.wait()
        num = num + num_held[other]
        den = den + den_held[other]
    out_ref[...] = num / (den + RIDGE)


def collect(numerator, denominator, count):
    rows, width = numerator.shape
    share_rows = rows // count
    shape = (count, share_rows, width)
    return pl.pallas_call(
        functools.partial(collect_kernel, count),
        out_shape=jax.ShapeDtypeStruct((share_rows, width), jnp.float32),
        in_specs=[pl.BlockSpec(memory_space=pltpu.VMEM)] * 2,
        out_specs=pl.BlockSpec(memory_space=pltpu.VMEM),
        scratch_shapes=[pltpu.VMEM(shape, jnp.float32)] * 2
        + [pltpu.SemaphoreType.DMA((count,))] * 4,
        compiler_params=pltpu.CompilerParams(collective_id=1, has_side_effects=True),
        name="collect",
    )(numerator.reshape(shape), denominator.reshape(shape))


def split_parts(values, count):
    parts = []
    for _ in range(count - 1):
        high = values.astype(jnp.bfloat16)
        parts.append(high)
        values = values - high.astype(jnp.float32)
    parts.append(values.astype(jnp.bfloat16))
    return parts


def one_hot(found):
    return jnp.where(found, 1.0, 0.0).astype(jnp.bfloat16)


def contract(left, right, left_dim, right_dim):
    return lax.dot_general(
        left, right, (((left_dim,), (right_dim,)), ((), ())), preferred_element_type=jnp.float32
    )


def stream_kernel(
    row_count, col_count, near, lanes, chunk, fold,
    rows_ref, base_ref, gain_ref, first_ref, second_ref, weight_ref, table_ref, model_ref,
    out_ref, flag_ref,
    model, send_rows, send_labels, rank_ref, pos_ref, rows_in, base_in, over_in, label_v, label_s,
    column_ref, gain_parts, gain_rows, picked, c_table, c_rows, lookup, picks, sums, powers,
    parts, half_in, halves, final_in,
    base_send, base_recv, name_send, name_recv, over_recv, mark_recv, along_send, along_mark,
    across_send, across_mark, relay_send, relay_mark, gain_send, gain_recv,
    half_send, half_recv, final_send, final_recv, local_sem,
):
    devices = row_count * col_count
    count, width = rows_ref.shape
    half = width // 2
    blocks = count // LANES
    far = lanes - near
    table_rows = first_ref.shape[0]
    slots = table_rows * LANES
    slot_bits = slots.bit_length() - 1
    row_block = sums.shape[0]
    col_block = gain_parts.shape[0]
    share_rows = gain_ref.shape[0]
    pairs = col_count // 2
    my_row = lax.axis_index("arow")
    my_col = lax.axis_index("acol")
    me = my_row * col_count + my_col
    parity = lax.rem(my_col, 2)
    my_pair = my_col // 2
    partner = my_col + 1 - 2 * parity
    barrier = pltpu.get_barrier_semaphore()

    def place(index):
        return (index // col_count, lax.rem(index, col_count))

    def remote(src, dst, send, recv, to):
        return pltpu.make_async_remote_copy(
            src_ref=src, dst_ref=dst, send_sem=send, recv_sem=recv,
            device_id=to, device_id_type=MESH,
        )

    load = pltpu.make_async_copy(model_ref, model, local_sem.at[0])
    load.start()

    def greet(step, carry):
        pl.semaphore_signal(
            barrier, inc=1, device_id=place(lax.rem(me + step, devices)), device_id_type=MESH
        )
        return carry

    lax.fori_loop(1, devices, greet, 0)

    upper = one_hot(
        lax.broadcasted_iota(jnp.int32, (LANES, LANES), 0)
        < lax.broadcasted_iota(jnp.int32, (LANES, LANES), 1)
    )
    tile = lax.broadcasted_iota(jnp.int32, (devices, LANES), 0)
    before = jnp.zeros((devices, 1), jnp.float32)
    for block in range(blocks):
        hit = tile == base_ref[block : block + 1, :] >> slot_bits
        hits = jnp.where(hit, 1.0, 0.0)
        within = jnp.dot(hits.astype(jnp.bfloat16), upper, preferred_element_type=jnp.float32)
        ranking = jnp.sum(jnp.where(hit, within + before, 0.0), axis=0, keepdims=True)
        before = before + jnp.sum(hits, axis=1, keepdims=True)
        rank_ref[block : block + 1, :] = ranking.astype(jnp.int32)
    ranks = rank_ref[...]
    over = ranks >= near
    overs = one_hot(over)
    lower = one_hot(
        lax.broadcasted_iota(jnp.int32, (blocks, blocks), 0)
        > lax.broadcasted_iota(jnp.int32, (blocks, blocks), 1)
    )
    earlier = jnp.dot(lower, overs, preferred_element_type=jnp.float32)
    over_rank = jnp.dot(overs, upper, preferred_element_type=jnp.float32) + jnp.sum(
        earlier, axis=1, keepdims=True
    )
    over_spot = near + over_rank.astype(jnp.int32)
    lost = jnp.max(jnp.where(over & (over_spot >= lanes), 1.0, 0.0), axis=(0, 1), keepdims=True)
    over_at = jnp.where(over, over_spot, -1)
    pos_ref[...] = jnp.where(
        over,
        jnp.where(over_spot < lanes, devices * near + over_spot - near, -1),
        (base_ref[...] >> slot_bits) * near + ranks,
    )

    spots = lax.broadcasted_iota(jnp.int32, (LANES, LANES), 0)
    over_spots = lax.broadcasted_iota(jnp.int32, (lanes, LANES), 0)
    sub = lax.broadcasted_iota(jnp.int32, (8, LANES), 0)
    names = jnp.zeros((3 * devices, LANES), jnp.float32)
    marks = jnp.zeros((8, lanes), jnp.float32)
    for block in range(blocks):
        slot = base_ref[block : block + 1, :]
        owner = slot >> slot_bits
        high = ((slot & (slots - 1)) >> 6).astype(jnp.float32)
        low_bits = (slot & 63).astype(jnp.float32)
        hit = tile == owner
        pieces = jnp.concatenate(
            [jnp.where(hit, high, 0.0), jnp.where(hit, low_bits, 0.0), jnp.where(hit, 1.0, 0.0)],
            axis=0,
        ).astype(jnp.bfloat16)
        names = names + contract(pieces, one_hot(spots == ranks[block : block + 1, :]), 1, 1)
        whole = jnp.where(
            sub == 0,
            owner.astype(jnp.float32),
            jnp.where(sub == 1, high, jnp.where(sub == 2, low_bits, jnp.where(sub == 3, 1.0, 0.0))),
        ).astype(jnp.bfloat16)
        marks = marks + contract(
            whole, one_hot(over_spots == over_at[block : block + 1, :]), 1, 1
        )
    lane = lax.broadcasted_iota(jnp.int32, (devices, LANES), 1)
    label = names[:devices] * 64.0 + names[devices : 2 * devices]
    label = jnp.where(names[2 * devices :] > 0.5, label, float(slots))
    label = jnp.where(lane == LANES - 1, lost, label).astype(jnp.int32)
    for index in range(devices):
        send_labels[index] = label[index : index + 1, :]
    base_in[me] = send_labels[me]
    mark = marks[0:1] * float(slots) + marks[1:2] * 64.0 + marks[2:3]
    over_in[me] = jnp.where(marks[3:4] > 0.5, mark, -1.0).astype(jnp.int32)

    def arrange(first, size):
        at = lax.broadcasted_iota(jnp.int32, (size, LANES), 0) + first
        hot = jnp.concatenate(
            [one_hot(at == pos_ref[block : block + 1, :]) for block in range(blocks)], axis=1
        )
        return jnp.dot(hot, rows_ref[...], preferred_element_type=jnp.float32).astype(jnp.bfloat16)

    rows_in[me, near:, :] = arrange(devices * near, far)

    def arrange_tiles(step, carry):
        got = arrange(step * (fold * near), fold * near)
        send_rows[pl.ds(step * fold, fold)] = got.reshape(fold, near, width)
        return carry

    lax.fori_loop(0, devices // fold, arrange_tiles, 0)
    rows_in[me, :near, :] = send_rows[me]

    pl.semaphore_wait(barrier, devices - 1)

    def name_copy(to, slot):
        return remote(
            send_labels.at[to], base_in.at[slot], name_send.at[to], name_recv.at[slot], place(to)
        )

    def base_copy(to, slot):
        return remote(
            send_rows.at[to], rows_in.at[slot, pl.ds(0, near)],
            base_send.at[to], base_recv.at[slot], place(to),
        )

    def mark_copy(source, to, mark):
        return remote(over_in.at[source], over_in.at[source], mark, mark_recv.at[source], to)

    def over_copy(source, to, send):
        there = rows_in.at[source, pl.ds(near, far)]
        return remote(there, there, send, over_recv.at[source], to)

    def over_copies(source, to, send, mark):
        return mark_copy(source, to, mark), over_copy(source, to, send)

    def along(step):
        row = lax.rem(my_row + step, row_count)
        return over_copies(me, (row, my_col), along_send.at[step], along_mark.at[step])

    def across(source_row, step):
        to = (my_row, lax.rem(my_col + 2 * step, col_count))
        return over_copies(
            source_row * col_count + my_col, to,
            across_send.at[source_row, step], across_mark.at[source_row, step],
        )

    def relay(source):
        return over_copies(
            source, (my_row, partner), relay_send.at[source], relay_mark.at[source]
        )

    def start(copies):
        for copy in copies:
            copy.start()

    def arrived(copies):
        for copy in copies:
            copy.wait_recv()

    def sent(copies):
        for copy in copies:
            copy.wait_send()

    column = me // row_count
    part = lax.rem(me, row_count)

    def gain_copy(row, col, slot):
        return remote(
            gain_ref, column_ref.at[slot], gain_send.at[row], gain_recv.at[slot], (row, col)
        )

    for row in range(row_count):
        stays = jnp.logical_and(row == my_row, column == my_col)

        @pl.when(jnp.logical_not(stays))
        def _():
            gain_copy(row, column, part).start()

        @pl.when(stays)
        def _():
            column_ref[part] = gain_ref[...]

    for step in range(1, row_count):
        start(along(step))
    for step in range(1, pairs):
        start(across(my_row, step))
    start(relay(me))

    def send_names(step, carry):
        name_copy(lax.rem(me + step, devices), me).start()
        return carry

    lax.fori_loop(1, devices, send_names, 0)

    def send_base(step, carry):
        base_copy(lax.rem(me + step, devices), me).start()
        return carry

    lax.fori_loop(1, devices, send_base, 0)

    for slot in range(row_count):
        source = my_col * row_count + slot

        @pl.when(source != me)
        def _():
            gain_copy(0, my_col, slot).wait_recv()

    gains = column_ref[...].reshape(col_block, width)
    odd = (lax.broadcasted_iota(jnp.int32, (col_block, width), 0) & 1) == 1
    even_gain = split_parts(jnp.where(odd, 0.0, gains), 3)
    odd_gain = split_parts(jnp.where(odd, gains, 0.0), 3)
    for number in range(3):
        gain_parts[:, 2 * number * width : (2 * number + 1) * width] = even_gain[number]
        gain_parts[:, (2 * number + 1) * width : (2 * number + 2) * width] = odd_gain[number]
    seconds = lax.broadcasted_iota(jnp.int32, (col_block, LANES), 0)

    def spread_gains(number, carry):
        hot = jnp.concatenate(
            [
                one_hot(seconds == second_ref[pl.ds(number * (chunk // LANES) + k, 1), :])
                for k in range(chunk // LANES)
            ],
            axis=1,
        )
        got = contract(hot, gain_parts[...], 0, 0)
        gain_rows[pl.ds(pl.multiple_of(number * chunk, chunk), chunk), :] = (
            got[:, : 2 * width] + got[:, 2 * width : 4 * width]
        ) + got[:, 4 * width :]
        return carry

    lax.fori_loop(0, slots // chunk, spread_gains, 0)
    lookup[:table_rows, :] = (first_ref[...] >> 1).astype(jnp.float32).astype(jnp.bfloat16)
    lookup[table_rows:, :] = (
        (((first_ref[...] & 1) << WEIGHT_BITS) + weight_ref[...]).astype(jnp.float32)
    ).astype(jnp.bfloat16)

    for step in range(1, row_count):
        source_row = lax.rem(my_row + step, row_count)
        source = source_row * col_count + my_col
        arrived(relay(source))
        for other in range(1, pairs):
            start(across(source_row, other))
        start(relay(source))

    load.wait()
    low = lax.broadcasted_iota(jnp.int32, (chunk, width), 1) < half
    c_table[slots:, :] = jnp.zeros((c_table.shape[0] - slots, width), jnp.float32)

    def piece(number, carry):
        begin = number * chunk

        def fetch(group, carry):
            at = group * GROUP
            held = [
                model[table_ref[begin + at + k]].astype(jnp.float32) for k in range(GROUP)
            ]
            for k in range(GROUP):
                picked[pl.ds(2 * (at + k), 2), :] = held[k]
            return carry

        lax.fori_loop(0, chunk // GROUP, fetch, 0)
        at = pl.ds(pl.multiple_of(begin, chunk), chunk)
        m_even = picked[pl.ds(0, chunk, stride=2), :]
        m_odd = picked[pl.ds(1, chunk, stride=2), :]
        g_even = gain_rows[at, :width]
        g_odd = gain_rows[at, width:]
        a = m_even * g_even + m_odd * g_odd
        b = m_even * pltpu.roll(g_even, half, 1) + m_odd * pltpu.roll(g_odd, half, 1)
        c_table[at, :] = jnp.where(
            low, a + pltpu.roll(a, half, 1), pltpu.roll(b, half, 1) - b
        )
        return carry

    lax.fori_loop(0, slots // chunk, piece, 0)

    for step in range(1, pairs):
        for source_row in range(row_count):
            source = source_row * col_count + lax.rem(my_col + 2 * step, col_count)
            arrived(relay(source))
            start(relay(source))

    def name_arrived(step, carry):
        other = lax.rem(me + step, devices)
        name_copy(other, other).wait()
        return carry

    lax.fori_loop(1, devices, name_arrived, 0)
    for step in range(pairs):
        for source_row in range(row_count):
            source = source_row * col_count + lax.rem(partner + 2 * step, col_count)
            mark_copy(source, (my_row, partner), relay_mark.at[source]).wait_recv()
    flag_ref[...] = jnp.broadcast_to(
        jnp.max(base_in[...], axis=0)[:, LANES - 1 :], flag_ref.shape
    )
    lane = lax.broadcasted_iota(jnp.int32, (1, LANES), 1)
    batch = fold * lanes

    def name_rows(step, carry):
        labels = []
        for number in range(fold):
            source = step * fold + number
            there = over_in[source] - me * slots
            there = jnp.where((there >= 0) & (there < slots), there, slots)
            near_part = jnp.where(lane < near, base_in[source], there[:, :LANES])
            if lanes > LANES:
                near_part = jnp.concatenate([near_part, there[:, LANES:]], axis=1)
            near_part = jnp.clip(near_part, 0, slots)
            label_v[source] = near_part
            labels.append(near_part)
        label = jnp.concatenate(labels, axis=1)
        hot = one_hot(lax.broadcasted_iota(jnp.int32, (LANES, batch), 0) == (label & (LANES - 1)))
        found = jnp.dot(lookup[...], hot, preferred_element_type=jnp.float32)
        line = lax.broadcasted_iota(jnp.int32, (table_rows, batch), 0) == label >> 7
        upper_bits = jnp.sum(
            jnp.where(line, found[:table_rows], 0.0), axis=0, keepdims=True
        ).astype(jnp.int32)
        rest = jnp.sum(
            jnp.where(line, found[table_rows:], 0.0), axis=0, keepdims=True
        ).astype(jnp.int32)
        first = 2 * upper_bits + (rest >> WEIGHT_BITS)
        weight = (rest & ((1 << WEIGHT_BITS) - 1)).astype(jnp.float32)
        picks[step] = jnp.where(
            lax.broadcasted_iota(jnp.int32, (row_block, batch), 0) == first, weight, 0.0
        ).astype(jnp.bfloat16)
        return carry

    lax.fori_loop(0, devices // fold, name_rows, 0)
    to_scalar = pltpu.make_async_copy(label_v, label_s, local_sem.at[1])
    to_scalar.start()
    to_scalar.wait()

    def grab_source(source, carry):
        def grab(group, carry):
            at = group * GROUP
            held = [
                c_table[pl.ds(label_s[source, 0, at + k], 1), :] for k in range(GROUP)
            ]
            for k in range(GROUP):
                c_rows[pl.ds(source * lanes + at + k, 1), :] = held[k]
            return carry

        return lax.fori_loop(0, lanes // GROUP, grab, carry)

    lax.fori_loop(0, devices, grab_source, 0)
    low = lax.broadcasted_iota(jnp.int32, (batch, width), 1) < half
    powers[...] = jnp.zeros_like(powers)
    sums[...] = jnp.zeros_like(sums)

    def add_power(step, carry):
        c = c_rows[pl.ds(pl.multiple_of(step * batch, batch), batch), :]
        power = c * c
        power = power + pltpu.roll(power, half, 1)
        high = power.astype(jnp.bfloat16).astype(jnp.float32)
        values = jnp.where(low, high, power - high).astype(jnp.bfloat16)
        powers[...] += jnp.dot(picks[step], values, preferred_element_type=jnp.float32)
        return carry

    lax.fori_loop(0, devices // fold, add_power, 0)

    def base_arrived(step, carry):
        other = lax.rem(me + step, devices)
        base_copy(other, other).wait()
        return carry

    lax.fori_loop(1, devices, base_arrived, 0)
    for step in range(pairs):
        for source_row in range(row_count):
            source = source_row * col_count + lax.rem(partner + 2 * step, col_count)
            over_copy(source, (my_row, partner), relay_send.at[source]).wait_recv()

    def add_product(step, carry):
        c = c_rows[pl.ds(pl.multiple_of(step * batch, batch), batch), :]
        r = rows_in[pl.ds(step * fold, fold)].reshape(batch, width).astype(jnp.float32)
        turned = pltpu.roll(c, half, 1)
        product = jnp.where(low, c, turned) * r + jnp.where(low, -turned, c) * pltpu.roll(
            r, half, 1
        )
        values = jnp.concatenate(split_parts(product, 2), axis=1)
        sums[...] += jnp.dot(picks[step], values, preferred_element_type=jnp.float32)
        return carry

    lax.fori_loop(0, devices // fold, add_product, 0)

    numerator = sums[:, :width] + sums[:, width:]
    denominator = powers[...] + pltpu.roll(powers[...], half, 1)
    side = share_rows // 2
    low = lax.broadcasted_iota(jnp.int32, (side, width), 1) < half
    for col in range(col_count):
        at = col * share_rows
        parts[col % 2, col // 2, :share_rows, :] = numerator[at : at + share_rows]
        parts[col % 2, col // 2, share_rows:, :] = jnp.where(
            low, denominator[at : at + side], denominator[at + side : at + share_rows]
        )
    swap = remote(
        parts.at[1 - parity], half_in, half_send, half_recv, (my_row, partner)
    )
    swap.start()

    for step in range(1, row_count):
        sent(along(step))
    for source_row in range(row_count):
        for step in range(1, pairs):
            sent(across(source_row, step))
    for step in range(pairs):
        for source_row in range(row_count):
            source = source_row * col_count + lax.rem(my_col + 2 * step, col_count)
            sent(relay(source))
    for row in range(row_count):
        stays = jnp.logical_and(row == my_row, column == my_col)

        @pl.when(jnp.logical_not(stays))
        def _():
            gain_copy(row, column, part).wait_send()

    swap.wait()
    halves[...] = parts[parity] + half_in[...]

    def final_copy(to, slot):
        return remote(
            halves.at[to], final_in.at[slot], final_send.at[to], final_recv.at[slot],
            (my_row, 2 * to + parity),
        )

    for step in range(1, pairs):
        final_copy(lax.rem(my_pair + step, pairs), my_pair).start()
    total = halves[my_pair]
    for step in range(1, pairs):
        other = lax.rem(my_pair + step, pairs)
        final_copy(other, other).wait()
        total = total + final_in[other]
    held = total[share_rows:]
    turned = pltpu.roll(held, half, 1)
    out_ref[:side, :] = total[:side] / (jnp.where(low, held, turned) + RIDGE)
    out_ref[side:, :] = total[side:share_rows] / (jnp.where(low, turned, held) + RIDGE)


def stream(rows, baseline, gains, first, second, weight, table, model_vis, row_count, col_count):
    devices = row_count * col_count
    count, width = rows.shape
    row_block, col_block, _ = model_vis.shape
    slots = table.shape[0]
    share_rows = gains.shape[0]
    mean = count // devices
    capacity = 4 * mean
    lanes = -(-capacity // LANES) * LANES
    near = -(-3 * mean // 32) * 16
    far = lanes - near
    blocks = count // LANES
    pairs = row_block * col_block // 2
    total = devices * lanes
    chunk = min(512, slots)
    fold = 4
    half_count = col_count // 2
    piece = (half_count, share_rows + share_rows // 2, width)
    vmem = pl.BlockSpec(memory_space=pltpu.VMEM)
    dma = pltpu.SemaphoreType.DMA
    return pl.pallas_call(
        functools.partial(stream_kernel, row_count, col_count, near, lanes, chunk, fold),
        out_shape=(
            jax.ShapeDtypeStruct(gains.shape, jnp.float32),
            jax.ShapeDtypeStruct((8, LANES), jnp.int32),
        ),
        in_specs=[vmem] * 6
        + [pl.BlockSpec(memory_space=pltpu.SMEM), pl.BlockSpec(memory_space=pl.ANY)],
        out_specs=(vmem, vmem),
        scratch_shapes=[
            pltpu.VMEM((pairs, 2, width), jnp.bfloat16),
            pltpu.VMEM((devices, near, width), jnp.bfloat16),
            pltpu.VMEM((devices, 1, LANES), jnp.int32),
            pltpu.VMEM((blocks, LANES), jnp.int32),
            pltpu.VMEM((blocks, LANES), jnp.int32),
            pltpu.VMEM((devices, lanes, width), jnp.bfloat16),
            pltpu.VMEM((devices, 1, LANES), jnp.int32),
            pltpu.VMEM((devices, 1, lanes), jnp.int32),
            pltpu.VMEM((devices, 1, lanes), jnp.int32),
            pltpu.SMEM((devices, 1, lanes), jnp.int32),
            pltpu.VMEM((row_count, share_rows, width), jnp.float32),
            pltpu.VMEM((col_block, 6 * width), jnp.bfloat16),
            pltpu.VMEM((slots, 2 * width), jnp.float32),
            pltpu.VMEM((2 * chunk, width), jnp.float32),
            pltpu.VMEM((slots + 8, width), jnp.float32),
            pltpu.VMEM((total, width), jnp.float32),
            pltpu.VMEM((2 * slots // LANES, LANES), jnp.bfloat16),
            pltpu.VMEM((devices // fold, row_block, fold * lanes), jnp.bfloat16),
            pltpu.VMEM((row_block, 2 * width), jnp.float32),
            pltpu.VMEM((row_block, width), jnp.float32),
            pltpu.VMEM((2,) + piece, jnp.float32),
            pltpu.VMEM(piece, jnp.float32),
            pltpu.VMEM(piece, jnp.float32),
            pltpu.VMEM(piece, jnp.float32),
        ]
        + [dma((devices,))] * 6
        + [dma((row_count,))] * 2
        + [dma((row_count, half_count))] * 2
        + [dma((devices,))] * 2
        + [dma((row_count,))] * 2
        + [dma] * 2
        + [dma((half_count,))] * 2
        + [dma((2,))],
        compiler_params=pltpu.CompilerParams(
            collective_id=2, has_side_effects=True, vmem_limit_bytes=63 << 20
        ),
        name="stream",
    )(
        rows,
        baseline.reshape(blocks, LANES),
        gains,
        first.reshape(slots // LANES, LANES),
        second.reshape(slots // LANES, LANES),
        weight.reshape(slots // LANES, LANES),
        table,
        model_vis.reshape(pairs, 2, width),
    )


def padded(row_count, col_count, row_data, row_baseline, pair_table, lengths, model_vis, gains):
    devices = row_count * col_count
    slots = lengths.shape[0]
    capacity = 4 * row_data.shape[0] // devices
    row_block, col_block, width = model_vis.shape
    total = devices * capacity
    my_row = lax.axis_index("arow")
    my_col = lax.axis_index("acol")
    first = pair_table[:, 0] - my_row * row_block
    second = pair_table[:, 1] - my_col * col_block
    pair = first * (col_block // 2) + second // 2
    table = ((pair << WEIGHT_BITS) + lengths) * (2 * col_block) + 2 * second
    table = jnp.concatenate([table, jnp.zeros((LANES,), jnp.int32)])
    outgoing, labels = route(row_data, row_baseline, devices, capacity, slots)
    names, column_gains = share(
        labels.reshape(devices, 1, capacity), gains, row_count, col_count
    )
    outgoing, names = lax.optimization_barrier((outgoing, names))
    arrived = lax.all_to_all(
        outgoing.reshape(devices, capacity, width),
        ("arow", "acol"),
        split_axis=0,
        concat_axis=0,
        tiled=True,
    ).reshape(total, width)
    c, info = gather(
        names.reshape(total), table, model_vis, column_gains.reshape(col_block, width)
    )
    power = segment(power_kernel, "power", info, [c], row_block, col_block)
    product = segment(product_kernel, "product", info, [c, arrived], row_block, col_block)
    return collect(product, power, col_count)


def local(row_count, col_count, row_data, row_baseline, pair_table, lengths, model_vis, gains):
    row_block, col_block, _ = model_vis.shape
    first = pair_table[:, 0] - lax.axis_index("arow") * row_block
    second = pair_table[:, 1] - lax.axis_index("acol") * col_block
    table = first * (col_block // 2) + second // 2
    updated, flag = stream(
        row_data, row_baseline, gains, first, second, lengths, table, model_vis,
        row_count, col_count,
    )
    return lax.cond(
        flag[0, 0] > 0,
        lambda: padded(
            row_count, col_count, row_data, row_baseline, pair_table, lengths, model_vis, gains
        ),
        lambda: updated,
    )


def solution(mesh):
    placed = (
        P(("arow", "acol"), None),
        P(("arow", "acol")),
        P(("arow", "acol"), None),
        P(("arow", "acol")),
        P("arow", "acol", None),
        P(("arow", "acol"), None),
    )
    return jax.shard_map(
        functools.partial(local, mesh.shape["arow"], mesh.shape["acol"]),
        mesh=mesh,
        in_specs=placed,
        out_specs=P(("arow", "acol"), None),
        check_vma=False,
    )
```

```python
import functools

import jax
import jax.numpy as jnp
from jax import lax
from jax.experimental import pallas as pl
from jax.experimental.pallas import tpu as pltpu
from jax.sharding import PartitionSpec as P

RIDGE = 1.0
LANES = 128
GROUP = 32
WEIGHT_BITS = 4
MESH = pl.DeviceIdType.MESH


def rows_at(ref, start, count):
    return ref[pl.ds(start, count), :]


def route_kernel(
    devices, capacity, slots, rows_ref, base_ref, out_ref, label_ref,
    wide, spread, target, local_id, empty, target_s, local_s, sems,
):
    blocks = base_ref.shape[0]
    count = rows_ref.shape[0]
    empty[...] = jnp.full(empty.shape, slots, jnp.int32)
    fill = pltpu.make_async_copy(empty, label_ref, sems.at[0])
    fill.start()
    order = lax.broadcasted_iota(jnp.int32, (LANES, LANES), 0)
    upper = (order < lax.broadcasted_iota(jnp.int32, (LANES, LANES), 1)).astype(jnp.bfloat16)
    tile = lax.broadcasted_iota(jnp.int32, (devices, LANES), 0)
    before = jnp.zeros((devices, 1), jnp.float32)
    for block in range(blocks):
        slot = base_ref[block : block + 1, :]
        owner = slot // slots
        hit = tile == owner
        hits = jnp.where(hit, 1.0, 0.0)
        within = jnp.dot(hits.astype(jnp.bfloat16), upper, preferred_element_type=jnp.float32)
        ranking = jnp.sum(jnp.where(hit, within + before, 0.0), axis=0, keepdims=True)
        before = before + jnp.sum(hits, axis=1, keepdims=True)
        target[block : block + 1, :] = owner * capacity + ranking.astype(jnp.int32)
        local_id[block : block + 1, :] = slot - owner * slots
    to_target = pltpu.make_async_copy(target, target_s, sems.at[1])
    to_target.start()
    to_local = pltpu.make_async_copy(local_id, local_s, sems.at[2])
    to_local.start()
    wide[...] = rows_ref[...].astype(jnp.float32)
    spread[...] = jnp.zeros_like(spread)
    to_target.wait()
    to_local.wait()
    fill.wait()

    def place_block(block, carry):
        def place(group, carry):
            first = group * GROUP
            spots = [target_s[block, first + k] for k in range(GROUP)]
            ids = [local_s[block, first + k] for k in range(GROUP)]
            held = [
                wide[pl.ds(block * LANES + first + k, 1), :] for k in range(GROUP)
            ]
            for k in range(GROUP):
                label_ref[spots[k]] = ids[k]
                spread[pl.ds(spots[k], 1), :] = held[k]
            return carry

        return lax.fori_loop(0, LANES // GROUP, place, carry)

    lax.fori_loop(0, count // LANES, place_block, 0)
    out_ref[...] = spread[...].astype(jnp.bfloat16)


def route(rows, baseline, devices, capacity, slots):
    count, width = rows.shape
    blocks = count // LANES
    total = devices * capacity
    return pl.pallas_call(
        functools.partial(route_kernel, devices, capacity, slots),
        out_shape=(
            jax.ShapeDtypeStruct((total, width), jnp.bfloat16),
            jax.ShapeDtypeStruct((total,), jnp.int32),
        ),
        in_specs=[pl.BlockSpec(memory_space=pltpu.VMEM)] * 2,
        out_specs=(
            pl.BlockSpec(memory_space=pltpu.VMEM),
            pl.BlockSpec(memory_space=pltpu.SMEM),
        ),
        scratch_shapes=[
            pltpu.VMEM((count, width), jnp.float32),
            pltpu.VMEM((total, width), jnp.float32),
            pltpu.VMEM((blocks, LANES), jnp.int32),
            pltpu.VMEM((blocks, LANES), jnp.int32),
            pltpu.VMEM((total,), jnp.int32),
            pltpu.SMEM((blocks, LANES), jnp.int32),
            pltpu.SMEM((blocks, LANES), jnp.int32),
            pltpu.SemaphoreType.DMA((3,)),
        ],
        name="route",
    )(rows, baseline.reshape(blocks, LANES))


def share_kernel(
    row_count, col_count, label_ref, gain_ref, name_ref, column_ref,
    send_sem, recv_sem, gain_send, gain_recv, local_sem,
):
    devices = row_count * col_count
    my_row = lax.axis_index("arow")
    my_col = lax.axis_index("acol")
    me = my_row * col_count + my_col
    barrier = pltpu.get_barrier_semaphore()

    def place(index):
        return (index // col_count, lax.rem(index, col_count))

    def greet(step, carry):
        pl.semaphore_signal(
            barrier, inc=1, device_id=place(lax.rem(me + step, devices)), device_id_type=MESH
        )
        return carry

    lax.fori_loop(1, devices, greet, 0)
    own = pltpu.make_async_copy(label_ref.at[me], name_ref.at[me], local_sem.at[0])
    own.start()
    pl.semaphore_wait(barrier, devices - 1)

    def label_copy(to, slot):
        return pltpu.make_async_remote_copy(
            src_ref=label_ref.at[to],
            dst_ref=name_ref.at[slot],
            send_sem=send_sem.at[to],
            recv_sem=recv_sem.at[slot],
            device_id=place(to),
            device_id_type=MESH,
        )

    def send(step, carry):
        label_copy(lax.rem(me + step, devices), me).start()
        return carry

    lax.fori_loop(1, devices, send, 0)
    column = me // row_count
    part = lax.rem(me, row_count)

    def gain_copy(row, col, slot):
        return pltpu.make_async_remote_copy(
            src_ref=gain_ref,
            dst_ref=column_ref.at[slot],
            send_sem=gain_send.at[row],
            recv_sem=gain_recv.at[slot],
            device_id=(row, col),
            device_id_type=MESH,
        )

    own_gain = pltpu.make_async_copy(gain_ref, column_ref.at[part], local_sem.at[1])
    for row in range(row_count):
        stays = jnp.logical_and(row == my_row, column == my_col)

        @pl.when(jnp.logical_not(stays))
        def _():
            gain_copy(row, column, part).start()

        @pl.when(stays)
        def _():
            own_gain.start()

    for row in range(row_count):
        stays = jnp.logical_and(row == my_row, column == my_col)

        @pl.when(jnp.logical_not(stays))
        def _():
            gain_copy(row, column, part).wait_send()

        @pl.when(stays)
        def _():
            own_gain.wait()

    for slot in range(row_count):
        source = my_col * row_count + slot

        @pl.when(source != me)
        def _():
            gain_copy(0, my_col, slot).wait_recv()

    def finish(step, carry):
        other = lax.rem(me + step, devices)
        label_copy(other, other).wait()
        return carry

    lax.fori_loop(1, devices, finish, 0)
    own.wait()


def share(labels, gains, row_count, col_count):
    devices = row_count * col_count
    return pl.pallas_call(
        functools.partial(share_kernel, row_count, col_count),
        out_shape=(
            jax.ShapeDtypeStruct(labels.shape, jnp.int32),
            jax.ShapeDtypeStruct((row_count,) + gains.shape, jnp.float32),
        ),
        in_specs=[pl.BlockSpec(memory_space=pltpu.VMEM)] * 2,
        out_specs=(pl.BlockSpec(memory_space=pltpu.VMEM),) * 2,
        scratch_shapes=[
            pltpu.SemaphoreType.DMA((devices,)),
            pltpu.SemaphoreType.DMA((devices,)),
            pltpu.SemaphoreType.DMA((row_count,)),
            pltpu.SemaphoreType.DMA((row_count,)),
            pltpu.SemaphoreType.DMA((2,)),
        ],
        compiler_params=pltpu.CompilerParams(collective_id=0, has_side_effects=True),
        name="share",
    )(labels, gains)


def gather_kernel(
    col_block, chunk, name_ref, table_ref, model_ref, gain_ref, c_ref, info_ref,
    model, pair_gain, gain_rows, picked, sem,
):
    total = c_ref.shape[0]
    width = c_ref.shape[1]
    half = width // 2
    load = pltpu.make_async_copy(model_ref, model, sem)
    load.start()
    shift = col_block.bit_length() + WEIGHT_BITS
    odd = lax.broadcasted_iota(jnp.int32, gain_ref.shape, 0) & 1
    pair_gain[pl.ds(0, col_block, stride=2), :] = jnp.where(odd == 0, gain_ref[...], 0.0)
    pair_gain[pl.ds(1, col_block, stride=2), :] = jnp.where(odd == 1, gain_ref[...], 0.0)

    def look(group, carry):
        first = group * GROUP
        names = [name_ref[first + k] for k in range(GROUP)]
        infos = [table_ref[name] for name in names]
        held = [pair_gain[pl.ds(info & (2 * col_block - 1), 2), :] for info in infos]
        for k in range(GROUP):
            info_ref[first + k] = infos[k]
            gain_rows[pl.ds(2 * (first + k), 2), :] = held[k]
        return carry

    lax.fori_loop(0, total // GROUP, look, 0)
    load.wait()

    def piece(number, carry):
        start = number * chunk

        def fetch(group, carry):
            first = group * GROUP
            infos = [info_ref[start + first + k] for k in range(GROUP)]
            held = [model[info >> shift].astype(jnp.float32) for info in infos]
            for k in range(GROUP):
                picked[pl.ds(2 * (first + k), 2), :] = held[k]
            return carry

        lax.fori_loop(0, chunk // GROUP, fetch, 0)
        at = pl.multiple_of(2 * start, 2 * chunk)
        m_even = picked[pl.ds(0, chunk, stride=2), :]
        m_odd = picked[pl.ds(1, chunk, stride=2), :]
        g_even = gain_rows[pl.ds(at, chunk, stride=2), :]
        g_odd = gain_rows[pl.ds(at + 1, chunk, stride=2), :]
        a = m_even * g_even + m_odd * g_odd
        b = m_even * pltpu.roll(g_even, half, 1) + m_odd * pltpu.roll(g_odd, half, 1)
        low = lax.broadcasted_iota(jnp.int32, (chunk, width), 1) < half
        c_ref[pl.ds(pl.multiple_of(start, chunk), chunk), :] = jnp.where(
            low, a + pltpu.roll(a, half, 1), pltpu.roll(b, half, 1) - b
        )
        return carry

    lax.fori_loop(0, total // chunk, piece, 0)


def gather(names, table, model_vis, column_gains):
    row_block, col_block, width = model_vis.shape
    pairs = row_block * col_block // 2
    total = names.shape[0]
    chunk = min(512, total)
    return pl.pallas_call(
        functools.partial(gather_kernel, col_block, chunk),
        out_shape=(
            jax.ShapeDtypeStruct((total, width), jnp.float32),
            jax.ShapeDtypeStruct((total,), jnp.int32),
        ),
        in_specs=[
            pl.BlockSpec(memory_space=pltpu.SMEM),
            pl.BlockSpec(memory_space=pltpu.SMEM),
            pl.BlockSpec(memory_space=pl.ANY),
            pl.BlockSpec(memory_space=pltpu.VMEM),
        ],
        out_specs=(
            pl.BlockSpec(memory_space=pltpu.VMEM),
            pl.BlockSpec(memory_space=pltpu.SMEM),
        ),
        scratch_shapes=[
            pltpu.VMEM((pairs, 2, width), jnp.bfloat16),
            pltpu.VMEM((2 * col_block, width), jnp.float32),
            pltpu.VMEM((2 * total, width), jnp.float32),
            pltpu.VMEM((2 * chunk, width), jnp.float32),
            pltpu.SemaphoreType.DMA,
        ],
        compiler_params=pltpu.CompilerParams(vmem_limit_bytes=56 << 20),
        cost_estimate=pl.CostEstimate(
            flops=1 << 20, bytes_accessed=model_vis.size * 2, transcendentals=0
        ),
        name="gather",
    )(names, table, model_vis.reshape(pairs, 2, width), column_gains)


def pick_rows(info, row_block, col_block):
    column_bits = col_block.bit_length()
    first = info >> (2 * column_bits + WEIGHT_BITS - 2)
    weight = ((info >> column_bits) & ((1 << WEIGHT_BITS) - 1)).astype(jnp.float32)
    spots = lax.broadcasted_iota(jnp.int32, (row_block, info.shape[1]), 0)
    return jnp.where(spots == first, weight, 0.0).astype(jnp.bfloat16)


def power_kernel(col_block, info_ref, c_ref, out_ref):
    row_block, width = out_ref.shape
    half = width // 2

    @pl.when(pl.program_id(0) == 0)
    def _():
        out_ref[...] = jnp.zeros_like(out_ref)

    c = c_ref[...]
    power = c * c
    power = power + pltpu.roll(power, half, 1)
    high = power.astype(jnp.bfloat16).astype(jnp.float32)
    low = lax.broadcasted_iota(jnp.int32, power.shape, 1) < half
    values = jnp.where(low, high, power - high).astype(jnp.bfloat16)
    sums = jnp.dot(
        pick_rows(info_ref[0], row_block, col_block), values, preferred_element_type=jnp.float32
    )
    out_ref[...] += sums + pltpu.roll(sums, half, 1)


def product_kernel(col_block, info_ref, c_ref, rows_ref, out_ref):
    row_block, width = out_ref.shape
    half = width // 2

    @pl.when(pl.program_id(0) == 0)
    def _():
        out_ref[...] = jnp.zeros_like(out_ref)

    c = c_ref[...]
    r = rows_ref[...].astype(jnp.float32)
    a = c * r
    b = c * pltpu.roll(r, half, 1)
    low = lax.broadcasted_iota(jnp.int32, c.shape, 1) < half
    product = jnp.where(low, a - pltpu.roll(a, half, 1), b + pltpu.roll(b, half, 1))
    high = product.astype(jnp.bfloat16)
    rest = (product - high.astype(jnp.float32)).astype(jnp.bfloat16)
    values = jnp.concatenate([high, rest], axis=1)
    sums = jnp.dot(
        pick_rows(info_ref[0], row_block, col_block), values, preferred_element_type=jnp.float32
    )
    out_ref[...] += sums[:, :width] + sums[:, width:]


def segment(kernel, name, info, arrays, row_block, col_block):
    total, width = arrays[0].shape
    chunk = min(1024, total)
    steps = total // chunk
    return pl.pallas_call(
        functools.partial(kernel, col_block),
        out_shape=jax.ShapeDtypeStruct((row_block, width), jnp.float32),
        grid=(steps,),
        in_specs=[pl.BlockSpec((1, 1, chunk), lambda i: (i, 0, 0))]
        + [pl.BlockSpec((chunk, width), lambda i: (i, 0))] * len(arrays),
        out_specs=pl.BlockSpec((row_block, width), lambda i: (0, 0)),
        cost_estimate=pl.CostEstimate(
            flops=2 * row_block * total * 2 * width,
            bytes_accessed=total * width * 4,
            transcendentals=0,
        ),
        name=name,
    )(info.reshape(steps, 1, chunk), *arrays)


def collect_kernel(
    count, num_ref, den_ref, out_ref, num_held, den_held, num_send, num_recv, den_send, den_recv
):
    me = lax.axis_index("acol")
    barrier = pltpu.get_barrier_semaphore()
    for step in range(1, count):
        pl.semaphore_signal(
            barrier,
            inc=1,
            device_id=(lax.axis_index("arow"), lax.rem(me + step, count)),
            device_id_type=MESH,
        )
    pl.semaphore_wait(barrier, count - 1)

    def copies(to, slot):
        return [
            pltpu.make_async_remote_copy(
                src_ref=part.at[to],
                dst_ref=held.at[slot],
                send_sem=send.at[to],
                recv_sem=recv.at[slot],
                device_id=(lax.axis_index("arow"), to),
                device_id_type=MESH,
            )
            for part, held, send, recv in (
                (den_ref, den_held, den_send, den_recv),
                (num_ref, num_held, num_send, num_recv),
            )
        ]

    for step in range(1, count):
        for copy in copies(lax.rem(me + step, count), me):
            copy.start()
    num = num_ref[me]
    den = den_ref[me]
    for step in range(1, count):
        other = lax.rem(me + step, count)
        for copy in copies(other, other):
            copy.wait()
        num = num + num_held[other]
        den = den + den_held[other]
    out_ref[...] = num / (den + RIDGE)


def collect(numerator, denominator, count):
    rows, width = numerator.shape
    share_rows = rows // count
    shape = (count, share_rows, width)
    return pl.pallas_call(
        functools.partial(collect_kernel, count),
        out_shape=jax.ShapeDtypeStruct((share_rows, width), jnp.float32),
        in_specs=[pl.BlockSpec(memory_space=pltpu.VMEM)] * 2,
        out_specs=pl.BlockSpec(memory_space=pltpu.VMEM),
        scratch_shapes=[pltpu.VMEM(shape, jnp.float32)] * 2
        + [pltpu.SemaphoreType.DMA((count,))] * 4,
        compiler_params=pltpu.CompilerParams(collective_id=1, has_side_effects=True),
        name="collect",
    )(numerator.reshape(shape), denominator.reshape(shape))


def split_parts(values, count):
    parts = []
    for _ in range(count - 1):
        high = values.astype(jnp.bfloat16)
        parts.append(high)
        values = values - high.astype(jnp.float32)
    parts.append(values.astype(jnp.bfloat16))
    return parts


def one_hot(found):
    return jnp.where(found, 1.0, 0.0).astype(jnp.bfloat16)


def contract(left, right, left_dim, right_dim):
    return lax.dot_general(
        left, right, (((left_dim,), (right_dim,)), ((), ())), preferred_element_type=jnp.float32
    )


def stream_kernel(
    row_count, col_count, near, lanes, chunk, fold,
    rows_ref, base_ref, gain_ref, pair_ref, weight_ref, model_ref,
    out_ref, flag_ref,
    model, send_rows, send_labels, rank_ref, pos_ref, rows_in, base_in, over_in, label_v, label_s,
    table_v, table_s, first_ref, second_ref,
    column_ref, gain_parts, gain_rows, picked, c_table, c_rows, lookup, firsts, weights, sums,
    parts, half_in, halves, final_in,
    base_send, base_recv, name_send, name_recv, over_send, mark_send, over_recv, mark_recv,
    half_send, half_recv, final_send, final_recv, gain_send, gain_recv, local_sem,
):
    devices = row_count * col_count
    count, width = rows_ref.shape
    half = width // 2
    blocks = count // LANES
    far = lanes - near
    table_rows = weight_ref.shape[0]
    slots = table_rows * LANES
    slot_bits = slots.bit_length() - 1
    row_block = sums.shape[0]
    col_block = gain_parts.shape[0]
    share_rows = gain_ref.shape[0]
    pairs = col_count // 2
    my_row = lax.axis_index("arow")
    my_col = lax.axis_index("acol")
    me = my_row * col_count + my_col
    parity = lax.rem(my_col, 2)
    my_pair = my_col // 2
    partner = my_col + 1 - 2 * parity
    barrier = pltpu.get_barrier_semaphore()

    def place(index):
        return (index // col_count, lax.rem(index, col_count))

    def remote(src, dst, send, recv, to):
        return pltpu.make_async_remote_copy(
            src_ref=src, dst_ref=dst, send_sem=send, recv_sem=recv,
            device_id=to, device_id_type=MESH,
        )

    load = pltpu.make_async_copy(model_ref, model, local_sem.at[0])
    load.start()

    def greet(step, carry):
        pl.semaphore_signal(
            barrier, inc=1, device_id=place(lax.rem(me + step, devices)), device_id_type=MESH
        )
        return carry

    lax.fori_loop(1, devices, greet, 0)
    for line in range(table_rows):
        first_ref[line : line + 1, :] = jnp.clip(
            pair_ref[line, 0:1, :] - my_row * row_block, 0, row_block - 1
        )
        second_ref[line : line + 1, :] = jnp.clip(
            pair_ref[line, 1:2, :] - my_col * col_block, 0, col_block - 1
        )
    table_v[...] = first_ref[...] * (col_block // 2) + (second_ref[...] >> 1)

    upper = one_hot(
        lax.broadcasted_iota(jnp.int32, (LANES, LANES), 0)
        < lax.broadcasted_iota(jnp.int32, (LANES, LANES), 1)
    )
    tile = lax.broadcasted_iota(jnp.int32, (devices, LANES), 0)
    before = jnp.zeros((devices, 1), jnp.float32)
    for block in range(blocks):
        hit = tile == base_ref[block : block + 1, :] >> slot_bits
        hits = jnp.where(hit, 1.0, 0.0)
        within = jnp.dot(hits.astype(jnp.bfloat16), upper, preferred_element_type=jnp.float32)
        ranking = jnp.sum(jnp.where(hit, within + before, 0.0), axis=0, keepdims=True)
        before = before + jnp.sum(hits, axis=1, keepdims=True)
        rank_ref[block : block + 1, :] = ranking.astype(jnp.int32)
    ranks = rank_ref[...]
    over = ranks >= near
    overs = one_hot(over)
    lower = one_hot(
        lax.broadcasted_iota(jnp.int32, (blocks, blocks), 0)
        > lax.broadcasted_iota(jnp.int32, (blocks, blocks), 1)
    )
    earlier = jnp.dot(lower, overs, preferred_element_type=jnp.float32)
    over_rank = jnp.dot(overs, upper, preferred_element_type=jnp.float32) + jnp.sum(
        earlier, axis=1, keepdims=True
    )
    over_spot = near + over_rank.astype(jnp.int32)
    lost = jnp.max(jnp.where(over & (over_spot >= lanes), 1.0, 0.0), axis=(0, 1), keepdims=True)
    over_at = jnp.where(over, over_spot, -1)
    pos_ref[...] = jnp.where(
        over,
        jnp.where(over_spot < lanes, devices * near + over_spot - near, -1),
        (base_ref[...] >> slot_bits) * near + ranks,
    )

    spots = lax.broadcasted_iota(jnp.int32, (LANES, LANES), 0)
    over_spots = lax.broadcasted_iota(jnp.int32, (lanes, LANES), 0)
    sub = lax.broadcasted_iota(jnp.int32, (8, LANES), 0)
    names = jnp.zeros((3 * devices, LANES), jnp.float32)
    marks = jnp.zeros((8, lanes), jnp.float32)
    for block in range(blocks):
        slot = base_ref[block : block + 1, :]
        owner = slot >> slot_bits
        high = ((slot & (slots - 1)) >> 6).astype(jnp.float32)
        low_bits = (slot & 63).astype(jnp.float32)
        hit = tile == owner
        pieces = jnp.concatenate(
            [jnp.where(hit, high, 0.0), jnp.where(hit, low_bits, 0.0), jnp.where(hit, 1.0, 0.0)],
            axis=0,
        ).astype(jnp.bfloat16)
        names = names + contract(pieces, one_hot(spots == ranks[block : block + 1, :]), 1, 1)
        whole = jnp.where(
            sub == 0,
            owner.astype(jnp.float32),
            jnp.where(sub == 1, high, jnp.where(sub == 2, low_bits, jnp.where(sub == 3, 1.0, 0.0))),
        ).astype(jnp.bfloat16)
        marks = marks + contract(
            whole, one_hot(over_spots == over_at[block : block + 1, :]), 1, 1
        )
    lane = lax.broadcasted_iota(jnp.int32, (devices, LANES), 1)
    label = names[:devices] * 64.0 + names[devices : 2 * devices]
    label = jnp.where(names[2 * devices :] > 0.5, label, float(slots))
    label = jnp.where(lane == LANES - 1, lost, label).astype(jnp.int32)
    for index in range(devices):
        send_labels[index] = label[index : index + 1, :]
    base_in[me] = send_labels[me]
    mark = marks[0:1] * float(slots) + marks[1:2] * 64.0 + marks[2:3]
    over_in[me] = jnp.where(marks[3:4] > 0.5, mark, -1.0).astype(jnp.int32)

    def arrange(first, size):
        at = lax.broadcasted_iota(jnp.int32, (size, LANES), 0) + first
        hot = jnp.concatenate(
            [one_hot(at == pos_ref[block : block + 1, :]) for block in range(blocks)], axis=1
        )
        return jnp.dot(hot, rows_ref[...], preferred_element_type=jnp.float32).astype(jnp.bfloat16)

    rows_in[me, near:, :] = arrange(devices * near, far)

    def arrange_tiles(step, carry):
        got = arrange(step * (fold * near), fold * near)
        send_rows[pl.ds(step * fold, fold)] = got.reshape(fold, near, width)
        return carry

    lax.fori_loop(0, devices // fold, arrange_tiles, 0)
    rows_in[me, :near, :] = send_rows[me]

    pl.semaphore_wait(barrier, devices - 1)

    def name_copy(to, slot):
        return remote(
            send_labels.at[to], base_in.at[slot], name_send, name_recv, place(to)
        )

    def base_copy(to, slot):
        return remote(
            send_rows.at[to], rows_in.at[slot, pl.ds(0, near)],
            base_send, base_recv, place(to),
        )

    def mark_copy(sources, to, stage):
        there = over_in.at[sources]
        return remote(there, there, mark_send, mark_recv.at[stage], to)

    def over_copy(sources, to, stage):
        there = rows_in.at[sources, pl.ds(near, far)]
        return remote(there, there, over_send, over_recv.at[stage], to)

    def over_copies(source, to, stage):
        return mark_copy(source, to, stage), over_copy(source, to, stage)

    def along(step):
        return over_copies(me, (lax.rem(my_row + step, row_count), my_col), 0)

    def across(source_row, step):
        to = (my_row, lax.rem(my_col + 2 * step, col_count))
        return over_copies(source_row * col_count + my_col, to, 1)

    def relay(source):
        return over_copies(source, (my_row, partner), 2)

    def start(copies):
        for copy in copies:
            copy.start()

    column = me // row_count
    part = lax.rem(me, row_count)

    def gain_copy(row, col, slot):
        return remote(
            gain_ref, column_ref.at[slot], gain_send.at[row], gain_recv.at[slot], (row, col)
        )

    for row in range(row_count):
        stays = jnp.logical_and(row == my_row, column == my_col)

        @pl.when(jnp.logical_not(stays))
        def _():
            gain_copy(row, column, part).start()

        @pl.when(stays)
        def _():
            column_ref[part] = gain_ref[...]

    for step in range(1, row_count):
        start(along(step))
    for step in range(1, pairs):
        start(across(my_row, step))
    start(relay(me))

    def send_names(step, carry):
        name_copy(lax.rem(me + step, devices), me).start()
        return carry

    lax.fori_loop(1, devices, send_names, 0)

    for slot in range(row_count):
        source = my_col * row_count + slot

        @pl.when(source != me)
        def _():
            gain_copy(0, my_col, slot).wait_recv()

    gains = split_parts(column_ref[...].reshape(col_block, width), 3)
    for number in range(3):
        gain_parts[:, number * width : (number + 1) * width] = gains[number]
    gain_parts[:, 3 * width :] = one_hot(
        (lax.broadcasted_iota(jnp.int32, (col_block, width), 0) & 1) == 1
    )
    seconds = lax.broadcasted_iota(jnp.int32, (col_block, LANES), 0)

    def spread_gains(number, carry):
        hot = jnp.concatenate(
            [
                one_hot(seconds == second_ref[pl.ds(number * (chunk // LANES) + k, 1), :])
                for k in range(chunk // LANES)
            ],
            axis=1,
        )
        got = contract(hot, gain_parts[...], 0, 0)
        at = pl.ds(pl.multiple_of(number * chunk, chunk), chunk)
        gain_rows[at, :width] = (got[:, :width] + got[:, width : 2 * width]) + got[
            :, 2 * width : 3 * width
        ]
        gain_rows[at, width:] = got[:, 3 * width :]
        return carry

    lax.fori_loop(0, slots // chunk, spread_gains, 0)
    to_table = pltpu.make_async_copy(table_v, table_s, local_sem.at[2])
    to_table.start()
    to_table.wait()
    lookup[:table_rows, :] = (first_ref[...] >> 1).astype(jnp.float32).astype(jnp.bfloat16)
    lookup[table_rows:, :] = (
        (((first_ref[...] & 1) << WEIGHT_BITS) + weight_ref[...]).astype(jnp.float32)
    ).astype(jnp.bfloat16)

    aside = (my_row, partner)
    mark_copy(pl.ds(0, row_count - 1), aside, 0).wait_recv()
    over_copy(pl.ds(0, row_count - 1), aside, 0).wait_recv()
    for step in range(1, row_count):
        source_row = lax.rem(my_row + step, row_count)
        for other in range(1, pairs):
            start(across(source_row, other))
        start(relay(source_row * col_count + my_col))

    def send_base(step, carry):
        base_copy(lax.rem(me + step, devices), me).start()
        return carry

    lax.fori_loop(1, devices, send_base, 0)

    load.wait()
    low = lax.broadcasted_iota(jnp.int32, (chunk, width), 1) < half
    c_table[slots:, :] = jnp.zeros((c_table.shape[0] - slots, width), jnp.float32)

    def piece(number, carry):
        begin = number * chunk

        def fetch(line, carry):
            to = pl.multiple_of(line * 2 * LANES, 2 * LANES)
            window = table_s.at[number * (chunk // LANES) + line]
            for at in range(0, LANES, GROUP):
                held = [model[window[at + k]].astype(jnp.float32) for k in range(GROUP)]
                for k in range(GROUP):
                    picked[pl.ds(to + 2 * (at + k), 2), :] = held[k]
            return carry

        lax.fori_loop(0, chunk // LANES, fetch, 0)
        at = pl.ds(pl.multiple_of(begin, chunk), chunk)
        m = jnp.where(
            gain_rows[at, width:] > 0.5,
            picked[pl.ds(1, chunk, stride=2), :],
            picked[pl.ds(0, chunk, stride=2), :],
        )
        g = gain_rows[at, :width]
        a = m * g
        b = m * pltpu.roll(g, half, 1)
        c_table[at, :] = jnp.where(
            low, a + pltpu.roll(a, half, 1), pltpu.roll(b, half, 1) - b
        )
        return carry

    lax.fori_loop(0, slots // chunk, piece, 0)

    mark_copy(pl.ds(0, row_count * (pairs - 1)), aside, 1).wait_recv()
    for step in range(1, pairs):
        for source_row in range(row_count):
            source = source_row * col_count + lax.rem(my_col + 2 * step, col_count)
            mark_copy(source, aside, 2).start()

    over_copy(pl.ds(0, row_count * (pairs - 1)), aside, 1).wait_recv()
    for step in range(1, pairs):
        for source_row in range(row_count):
            source = source_row * col_count + lax.rem(my_col + 2 * step, col_count)
            over_copy(source, aside, 2).start()

    remote(
        send_labels.at[pl.ds(0, devices - 1)], base_in.at[pl.ds(0, devices - 1)],
        name_send, name_recv, aside,
    ).wait()
    mark_copy(pl.ds(0, row_count * pairs), aside, 2).wait_recv()
    lane = lax.broadcasted_iota(jnp.int32, (devices, 1, LANES), 2)
    flag_ref[0, 0] = jnp.max(jnp.where(lane == LANES - 1, base_in[...], 0).astype(jnp.float32)).astype(
        jnp.int32
    )
    lane = lax.broadcasted_iota(jnp.int32, (1, LANES), 1)
    batch = fold * lanes

    def name_rows(step, carry):
        labels = []
        for number in range(fold):
            source = step * fold + number
            there = over_in[source] - me * slots
            there = jnp.where((there >= 0) & (there < slots), there, slots)
            near_part = jnp.where(lane < near, base_in[source], there[:, :LANES])
            if lanes > LANES:
                near_part = jnp.concatenate([near_part, there[:, LANES:]], axis=1)
            near_part = jnp.clip(near_part, 0, slots)
            for line in range(lanes // LANES):
                label_v[source * (lanes // LANES) + line] = near_part[
                    :, line * LANES : (line + 1) * LANES
                ]
            labels.append(near_part)
        label = jnp.concatenate(labels, axis=1)
        hot = one_hot(lax.broadcasted_iota(jnp.int32, (LANES, batch), 0) == (label & (LANES - 1)))
        found = jnp.dot(lookup[...], hot, preferred_element_type=jnp.float32)
        line = lax.broadcasted_iota(jnp.int32, (table_rows, batch), 0) == label >> 7
        upper_bits = jnp.sum(
            jnp.where(line, found[:table_rows], 0.0), axis=0, keepdims=True
        ).astype(jnp.int32)
        rest = jnp.sum(
            jnp.where(line, found[table_rows:], 0.0), axis=0, keepdims=True
        ).astype(jnp.int32)
        firsts[step] = 2 * upper_bits + (rest >> WEIGHT_BITS)
        weights[step] = (rest & ((1 << WEIGHT_BITS) - 1)).astype(jnp.float32)
        return carry

    lax.fori_loop(0, devices // fold, name_rows, 0)
    to_scalar = pltpu.make_async_copy(label_v, label_s, local_sem.at[1])
    to_scalar.start()
    to_scalar.wait()

    def grab(line, carry):
        to = pl.multiple_of(line * LANES, LANES)
        window = label_s.at[line, 0]
        for at in range(0, LANES, GROUP):
            held = [c_table[pl.ds(window[at + k], 1), :] for k in range(GROUP)]
            for k in range(GROUP):
                c_rows[pl.ds(to + at + k, 1), :] = held[k]
        return carry

    lax.fori_loop(0, devices * lanes // LANES, grab, 0)
    low = lax.broadcasted_iota(jnp.int32, (batch, width), 1) < half
    sums[...] = jnp.zeros_like(sums)

    remote(
        send_rows.at[pl.ds(0, devices - 1)], rows_in.at[pl.ds(0, devices - 1), pl.ds(0, near)],
        base_send, base_recv, aside,
    ).wait()
    over_copy(pl.ds(0, row_count * pairs), aside, 2).wait_recv()

    def add_product(step, carry):
        c = c_rows[pl.ds(pl.multiple_of(step * batch, batch), batch), :]
        r = rows_in[pl.ds(step * fold, fold)].reshape(batch, width).astype(jnp.float32)
        turned = pltpu.roll(c, half, 1)
        product = jnp.where(low, c, turned) * r + jnp.where(low, -turned, c) * pltpu.roll(
            r, half, 1
        )
        power = c * c
        power = power + pltpu.roll(power, half, 1)
        power_high = power.astype(jnp.bfloat16).astype(jnp.float32)
        power = jnp.where(low, power_high, power - power_high).astype(jnp.bfloat16)
        values = jnp.concatenate(split_parts(product, 2) + [power], axis=1)
        pick = jnp.where(
            lax.broadcasted_iota(jnp.int32, (row_block, batch), 0) == firsts[step],
            weights[step],
            0.0,
        ).astype(jnp.bfloat16)
        sums[...] += jnp.dot(pick, values, preferred_element_type=jnp.float32)
        return carry

    lax.fori_loop(0, devices // fold, add_product, 0)

    numerator = sums[:, :width] + sums[:, width : 2 * width]
    denominator = sums[:, 2 * width :]
    denominator = denominator + pltpu.roll(denominator, half, 1)
    side = share_rows // 2
    low = lax.broadcasted_iota(jnp.int32, (side, width), 1) < half
    for col in range(col_count):
        at = col * share_rows
        parts[col % 2, col // 2, :share_rows, :] = numerator[at : at + share_rows]
        parts[col % 2, col // 2, share_rows:, :] = jnp.where(
            low, denominator[at : at + side], denominator[at + side : at + share_rows]
        )
    swap = remote(
        parts.at[1 - parity], half_in, half_send, half_recv, (my_row, partner)
    )
    swap.start()

    mark_copy(pl.ds(0, devices - 1), aside, 0).wait_send()
    over_copy(pl.ds(0, devices - 1), aside, 0).wait_send()
    for row in range(row_count):
        stays = jnp.logical_and(row == my_row, column == my_col)

        @pl.when(jnp.logical_not(stays))
        def _():
            gain_copy(row, column, part).wait_send()

    swap.wait()
    halves[...] = parts[parity] + half_in[...]

    def final_copy(to, slot, device):
        return remote(halves.at[to], final_in.at[slot], final_send, final_recv, device)

    for step in range(1, pairs):
        to = lax.rem(my_pair + step, pairs)
        final_copy(to, my_pair, (my_row, 2 * to + parity)).start()
    final_copy(pl.ds(0, pairs - 1), pl.ds(0, pairs - 1), aside).wait()
    total = halves[my_pair]
    for step in range(1, pairs):
        total = total + final_in[lax.rem(my_pair + step, pairs)]
    held = total[share_rows:]
    turned = pltpu.roll(held, half, 1)
    out_ref[:side, :] = total[:side] / (jnp.where(low, held, turned) + RIDGE)
    out_ref[side:, :] = total[side:share_rows] / (jnp.where(low, turned, held) + RIDGE)


def stream(rows, baseline, gains, pair_table, weight, model_vis, row_count, col_count):
    devices = row_count * col_count
    count, width = rows.shape
    row_block, col_block, _ = model_vis.shape
    slots = weight.shape[0]
    share_rows = gains.shape[0]
    mean = count // devices
    capacity = 4 * mean
    lanes = -(-capacity // LANES) * LANES
    near = -(-3 * mean // 32) * 16
    far = lanes - near
    blocks = count // LANES
    pairs = row_block * col_block // 2
    total = devices * lanes
    chunk = min(512, slots)
    fold = 4
    half_count = col_count // 2
    piece = (half_count, share_rows + share_rows // 2, width)
    vmem = pl.BlockSpec(memory_space=pltpu.VMEM)
    dma = pltpu.SemaphoreType.DMA
    return pl.pallas_call(
        functools.partial(stream_kernel, row_count, col_count, near, lanes, chunk, fold),
        out_shape=(
            jax.ShapeDtypeStruct(gains.shape, jnp.float32),
            jax.ShapeDtypeStruct((1, 1), jnp.int32),
        ),
        in_specs=[vmem] * 5 + [pl.BlockSpec(memory_space=pl.ANY)],
        out_specs=(vmem, pl.BlockSpec(memory_space=pltpu.SMEM)),
        scratch_shapes=[
            pltpu.VMEM((pairs, 2, width), jnp.bfloat16),
            pltpu.VMEM((devices, near, width), jnp.bfloat16),
            pltpu.VMEM((devices, 1, LANES), jnp.int32),
            pltpu.VMEM((blocks, LANES), jnp.int32),
            pltpu.VMEM((blocks, LANES), jnp.int32),
            pltpu.VMEM((devices, lanes, width), jnp.bfloat16),
            pltpu.VMEM((devices, 1, LANES), jnp.int32),
            pltpu.VMEM((devices, 1, lanes), jnp.int32),
            pltpu.VMEM((total // LANES, 1, LANES), jnp.int32),
            pltpu.SMEM((total // LANES, 1, LANES), jnp.int32),
            pltpu.VMEM((slots // LANES, LANES), jnp.int32),
            pltpu.SMEM((slots // LANES, LANES), jnp.int32),
            pltpu.VMEM((slots // LANES, LANES), jnp.int32),
            pltpu.VMEM((slots // LANES, LANES), jnp.int32),
            pltpu.VMEM((row_count, share_rows, width), jnp.float32),
            pltpu.VMEM((col_block, 4 * width), jnp.bfloat16),
            pltpu.VMEM((slots, 2 * width), jnp.float32),
            pltpu.VMEM((2 * chunk, width), jnp.float32),
            pltpu.VMEM((slots + 8, width), jnp.float32),
            pltpu.VMEM((total, width), jnp.float32),
            pltpu.VMEM((2 * slots // LANES, LANES), jnp.bfloat16),
            pltpu.VMEM((devices // fold, 1, fold * lanes), jnp.int32),
            pltpu.VMEM((devices // fold, 1, fold * lanes), jnp.float32),
            pltpu.VMEM((row_block, 3 * width), jnp.float32),
            pltpu.VMEM((2,) + piece, jnp.float32),
            pltpu.VMEM(piece, jnp.float32),
            pltpu.VMEM(piece, jnp.float32),
            pltpu.VMEM(piece, jnp.float32),
        ]
        + [dma] * 6
        + [dma((3,))] * 2
        + [dma] * 4
        + [dma((row_count,))] * 2
        + [dma((3,))],
        compiler_params=pltpu.CompilerParams(
            collective_id=2, has_side_effects=True, vmem_limit_bytes=63 << 20
        ),
        name="stream",
    )(
        rows,
        baseline.reshape(blocks, LANES),
        gains,
        pair_table.reshape(slots // LANES, LANES, 2).transpose(0, 2, 1),
        weight.reshape(slots // LANES, LANES),
        model_vis.reshape(pairs, 2, width),
    )


def padded(row_count, col_count, row_data, row_baseline, pair_table, lengths, model_vis, gains):
    devices = row_count * col_count
    slots = lengths.shape[0]
    capacity = 4 * row_data.shape[0] // devices
    row_block, col_block, width = model_vis.shape
    total = devices * capacity
    my_row = lax.axis_index("arow")
    my_col = lax.axis_index("acol")
    first = pair_table[:, 0] - my_row * row_block
    second = pair_table[:, 1] - my_col * col_block
    pair = first * (col_block // 2) + second // 2
    table = ((pair << WEIGHT_BITS) + lengths) * (2 * col_block) + 2 * second
    table = jnp.concatenate([table, jnp.zeros((LANES,), jnp.int32)])
    outgoing, labels = route(row_data, row_baseline, devices, capacity, slots)
    names, column_gains = share(
        labels.reshape(devices, 1, capacity), gains, row_count, col_count
    )
    outgoing, names = lax.optimization_barrier((outgoing, names))
    arrived = lax.all_to_all(
        outgoing.reshape(devices, capacity, width),
        ("arow", "acol"),
        split_axis=0,
        concat_axis=0,
        tiled=True,
    ).reshape(total, width)
    c, info = gather(
        names.reshape(total), table, model_vis, column_gains.reshape(col_block, width)
    )
    power = segment(power_kernel, "power", info, [c], row_block, col_block)
    product = segment(product_kernel, "product", info, [c, arrived], row_block, col_block)
    return collect(product, power, col_count)


def local(row_count, col_count, row_data, row_baseline, pair_table, lengths, model_vis, gains):
    updated, flag = stream(
        row_data, row_baseline, gains, pair_table, lengths, model_vis, row_count, col_count
    )
    return lax.cond(
        flag[0, 0] > 0,
        lambda: padded(
            row_count, col_count, row_data, row_baseline, pair_table, lengths, model_vis, gains
        ),
        lambda: updated,
    )


def solution(mesh):
    placed = (
        P(("arow", "acol"), None),
        P(("arow", "acol")),
        P(("arow", "acol"), None),
        P(("arow", "acol")),
        P("arow", "acol", None),
        P(("arow", "acol"), None),
    )
    return jax.shard_map(
        functools.partial(local, mesh.shape["arow"], mesh.shape["acol"]),
        mesh=mesh,
        in_specs=placed,
        out_specs=P(("arow", "acol"), None),
        check_vma=False,
    )
```

```python
import functools

import jax
import jax.numpy as jnp
from jax import lax
from jax.experimental import pallas as pl
from jax.experimental.pallas import tpu as pltpu
from jax.sharding import PartitionSpec as P

RIDGE = 1.0
LANES = 128
GROUP = 32
WEIGHT_BITS = 4
MESH = pl.DeviceIdType.MESH


def rows_at(ref, start, count):
    return ref[pl.ds(start, count), :]


def route_kernel(
    devices, capacity, slots, rows_ref, base_ref, out_ref, label_ref,
    wide, spread, target, local_id, empty, target_s, local_s, sems,
):
    blocks = base_ref.shape[0]
    count = rows_ref.shape[0]
    empty[...] = jnp.full(empty.shape, slots, jnp.int32)
    fill = pltpu.make_async_copy(empty, label_ref, sems.at[0])
    fill.start()
    order = lax.broadcasted_iota(jnp.int32, (LANES, LANES), 0)
    upper = (order < lax.broadcasted_iota(jnp.int32, (LANES, LANES), 1)).astype(jnp.bfloat16)
    tile = lax.broadcasted_iota(jnp.int32, (devices, LANES), 0)
    before = jnp.zeros((devices, 1), jnp.float32)
    for block in range(blocks):
        slot = base_ref[block : block + 1, :]
        owner = slot // slots
        hit = tile == owner
        hits = jnp.where(hit, 1.0, 0.0)
        within = jnp.dot(hits.astype(jnp.bfloat16), upper, preferred_element_type=jnp.float32)
        ranking = jnp.sum(jnp.where(hit, within + before, 0.0), axis=0, keepdims=True)
        before = before + jnp.sum(hits, axis=1, keepdims=True)
        target[block : block + 1, :] = owner * capacity + ranking.astype(jnp.int32)
        local_id[block : block + 1, :] = slot - owner * slots
    to_target = pltpu.make_async_copy(target, target_s, sems.at[1])
    to_target.start()
    to_local = pltpu.make_async_copy(local_id, local_s, sems.at[2])
    to_local.start()
    wide[...] = rows_ref[...].astype(jnp.float32)
    spread[...] = jnp.zeros_like(spread)
    to_target.wait()
    to_local.wait()
    fill.wait()

    def place_block(block, carry):
        def place(group, carry):
            first = group * GROUP
            spots = [target_s[block, first + k] for k in range(GROUP)]
            ids = [local_s[block, first + k] for k in range(GROUP)]
            held = [
                wide[pl.ds(block * LANES + first + k, 1), :] for k in range(GROUP)
            ]
            for k in range(GROUP):
                label_ref[spots[k]] = ids[k]
                spread[pl.ds(spots[k], 1), :] = held[k]
            return carry

        return lax.fori_loop(0, LANES // GROUP, place, carry)

    lax.fori_loop(0, count // LANES, place_block, 0)
    out_ref[...] = spread[...].astype(jnp.bfloat16)


def route(rows, baseline, devices, capacity, slots):
    count, width = rows.shape
    blocks = count // LANES
    total = devices * capacity
    return pl.pallas_call(
        functools.partial(route_kernel, devices, capacity, slots),
        out_shape=(
            jax.ShapeDtypeStruct((total, width), jnp.bfloat16),
            jax.ShapeDtypeStruct((total,), jnp.int32),
        ),
        in_specs=[pl.BlockSpec(memory_space=pltpu.VMEM)] * 2,
        out_specs=(
            pl.BlockSpec(memory_space=pltpu.VMEM),
            pl.BlockSpec(memory_space=pltpu.SMEM),
        ),
        scratch_shapes=[
            pltpu.VMEM((count, width), jnp.float32),
            pltpu.VMEM((total, width), jnp.float32),
            pltpu.VMEM((blocks, LANES), jnp.int32),
            pltpu.VMEM((blocks, LANES), jnp.int32),
            pltpu.VMEM((total,), jnp.int32),
            pltpu.SMEM((blocks, LANES), jnp.int32),
            pltpu.SMEM((blocks, LANES), jnp.int32),
            pltpu.SemaphoreType.DMA((3,)),
        ],
        name="route",
    )(rows, baseline.reshape(blocks, LANES))


def share_kernel(
    row_count, col_count, label_ref, gain_ref, name_ref, column_ref,
    send_sem, recv_sem, gain_send, gain_recv, local_sem,
):
    devices = row_count * col_count
    my_row = lax.axis_index("arow")
    my_col = lax.axis_index("acol")
    me = my_row * col_count + my_col
    barrier = pltpu.get_barrier_semaphore()

    def place(index):
        return (index // col_count, lax.rem(index, col_count))

    def greet(step, carry):
        pl.semaphore_signal(
            barrier, inc=1, device_id=place(lax.rem(me + step, devices)), device_id_type=MESH
        )
        return carry

    lax.fori_loop(1, devices, greet, 0)
    own = pltpu.make_async_copy(label_ref.at[me], name_ref.at[me], local_sem.at[0])
    own.start()
    pl.semaphore_wait(barrier, devices - 1)

    def label_copy(to, slot):
        return pltpu.make_async_remote_copy(
            src_ref=label_ref.at[to],
            dst_ref=name_ref.at[slot],
            send_sem=send_sem.at[to],
            recv_sem=recv_sem.at[slot],
            device_id=place(to),
            device_id_type=MESH,
        )

    def send(step, carry):
        label_copy(lax.rem(me + step, devices), me).start()
        return carry

    lax.fori_loop(1, devices, send, 0)
    column = me // row_count
    part = lax.rem(me, row_count)

    def gain_copy(row, col, slot):
        return pltpu.make_async_remote_copy(
            src_ref=gain_ref,
            dst_ref=column_ref.at[slot],
            send_sem=gain_send.at[row],
            recv_sem=gain_recv.at[slot],
            device_id=(row, col),
            device_id_type=MESH,
        )

    own_gain = pltpu.make_async_copy(gain_ref, column_ref.at[part], local_sem.at[1])
    for row in range(row_count):
        stays = jnp.logical_and(row == my_row, column == my_col)

        @pl.when(jnp.logical_not(stays))
        def _():
            gain_copy(row, column, part).start()

        @pl.when(stays)
        def _():
            own_gain.start()

    for row in range(row_count):
        stays = jnp.logical_and(row == my_row, column == my_col)

        @pl.when(jnp.logical_not(stays))
        def _():
            gain_copy(row, column, part).wait_send()

        @pl.when(stays)
        def _():
            own_gain.wait()

    for slot in range(row_count):
        source = my_col * row_count + slot

        @pl.when(source != me)
        def _():
            gain_copy(0, my_col, slot).wait_recv()

    def finish(step, carry):
        other = lax.rem(me + step, devices)
        label_copy(other, other).wait()
        return carry

    lax.fori_loop(1, devices, finish, 0)
    own.wait()


def share(labels, gains, row_count, col_count):
    devices = row_count * col_count
    return pl.pallas_call(
        functools.partial(share_kernel, row_count, col_count),
        out_shape=(
            jax.ShapeDtypeStruct(labels.shape, jnp.int32),
            jax.ShapeDtypeStruct((row_count,) + gains.shape, jnp.float32),
        ),
        in_specs=[pl.BlockSpec(memory_space=pltpu.VMEM)] * 2,
        out_specs=(pl.BlockSpec(memory_space=pltpu.VMEM),) * 2,
        scratch_shapes=[
            pltpu.SemaphoreType.DMA((devices,)),
            pltpu.SemaphoreType.DMA((devices,)),
            pltpu.SemaphoreType.DMA((row_count,)),
            pltpu.SemaphoreType.DMA((row_count,)),
            pltpu.SemaphoreType.DMA((2,)),
        ],
        compiler_params=pltpu.CompilerParams(collective_id=0, has_side_effects=True),
        name="share",
    )(labels, gains)


def gather_kernel(
    col_block, chunk, name_ref, table_ref, model_ref, gain_ref, c_ref, info_ref,
    model, pair_gain, gain_rows, picked, sem,
):
    total = c_ref.shape[0]
    width = c_ref.shape[1]
    half = width // 2
    load = pltpu.make_async_copy(model_ref, model, sem)
    load.start()
    shift = col_block.bit_length() + WEIGHT_BITS
    odd = lax.broadcasted_iota(jnp.int32, gain_ref.shape, 0) & 1
    pair_gain[pl.ds(0, col_block, stride=2), :] = jnp.where(odd == 0, gain_ref[...], 0.0)
    pair_gain[pl.ds(1, col_block, stride=2), :] = jnp.where(odd == 1, gain_ref[...], 0.0)

    def look(group, carry):
        first = group * GROUP
        names = [name_ref[first + k] for k in range(GROUP)]
        infos = [table_ref[name] for name in names]
        held = [pair_gain[pl.ds(info & (2 * col_block - 1), 2), :] for info in infos]
        for k in range(GROUP):
            info_ref[first + k] = infos[k]
            gain_rows[pl.ds(2 * (first + k), 2), :] = held[k]
        return carry

    lax.fori_loop(0, total // GROUP, look, 0)
    load.wait()

    def piece(number, carry):
        start = number * chunk

        def fetch(group, carry):
            first = group * GROUP
            infos = [info_ref[start + first + k] for k in range(GROUP)]
            held = [model[info >> shift].astype(jnp.float32) for info in infos]
            for k in range(GROUP):
                picked[pl.ds(2 * (first + k), 2), :] = held[k]
            return carry

        lax.fori_loop(0, chunk // GROUP, fetch, 0)
        at = pl.multiple_of(2 * start, 2 * chunk)
        m_even = picked[pl.ds(0, chunk, stride=2), :]
        m_odd = picked[pl.ds(1, chunk, stride=2), :]
        g_even = gain_rows[pl.ds(at, chunk, stride=2), :]
        g_odd = gain_rows[pl.ds(at + 1, chunk, stride=2), :]
        a = m_even * g_even + m_odd * g_odd
        b = m_even * pltpu.roll(g_even, half, 1) + m_odd * pltpu.roll(g_odd, half, 1)
        low = lax.broadcasted_iota(jnp.int32, (chunk, width), 1) < half
        c_ref[pl.ds(pl.multiple_of(start, chunk), chunk), :] = jnp.where(
            low, a + pltpu.roll(a, half, 1), pltpu.roll(b, half, 1) - b
        )
        return carry

    lax.fori_loop(0, total // chunk, piece, 0)


def gather(names, table, model_vis, column_gains):
    row_block, col_block, width = model_vis.shape
    pairs = row_block * col_block // 2
    total = names.shape[0]
    chunk = min(512, total)
    return pl.pallas_call(
        functools.partial(gather_kernel, col_block, chunk),
        out_shape=(
            jax.ShapeDtypeStruct((total, width), jnp.float32),
            jax.ShapeDtypeStruct((total,), jnp.int32),
        ),
        in_specs=[
            pl.BlockSpec(memory_space=pltpu.SMEM),
            pl.BlockSpec(memory_space=pltpu.SMEM),
            pl.BlockSpec(memory_space=pl.ANY),
            pl.BlockSpec(memory_space=pltpu.VMEM),
        ],
        out_specs=(
            pl.BlockSpec(memory_space=pltpu.VMEM),
            pl.BlockSpec(memory_space=pltpu.SMEM),
        ),
        scratch_shapes=[
            pltpu.VMEM((pairs, 2, width), jnp.bfloat16),
            pltpu.VMEM((2 * col_block, width), jnp.float32),
            pltpu.VMEM((2 * total, width), jnp.float32),
            pltpu.VMEM((2 * chunk, width), jnp.float32),
            pltpu.SemaphoreType.DMA,
        ],
        compiler_params=pltpu.CompilerParams(vmem_limit_bytes=56 << 20),
        cost_estimate=pl.CostEstimate(
            flops=1 << 20, bytes_accessed=model_vis.size * 2, transcendentals=0
        ),
        name="gather",
    )(names, table, model_vis.reshape(pairs, 2, width), column_gains)


def pick_rows(info, row_block, col_block):
    column_bits = col_block.bit_length()
    first = info >> (2 * column_bits + WEIGHT_BITS - 2)
    weight = ((info >> column_bits) & ((1 << WEIGHT_BITS) - 1)).astype(jnp.float32)
    spots = lax.broadcasted_iota(jnp.int32, (row_block, info.shape[1]), 0)
    return jnp.where(spots == first, weight, 0.0).astype(jnp.bfloat16)


def power_kernel(col_block, info_ref, c_ref, out_ref):
    row_block, width = out_ref.shape
    half = width // 2

    @pl.when(pl.program_id(0) == 0)
    def _():
        out_ref[...] = jnp.zeros_like(out_ref)

    c = c_ref[...]
    power = c * c
    power = power + pltpu.roll(power, half, 1)
    high = power.astype(jnp.bfloat16).astype(jnp.float32)
    low = lax.broadcasted_iota(jnp.int32, power.shape, 1) < half
    values = jnp.where(low, high, power - high).astype(jnp.bfloat16)
    sums = jnp.dot(
        pick_rows(info_ref[0], row_block, col_block), values, preferred_element_type=jnp.float32
    )
    out_ref[...] += sums + pltpu.roll(sums, half, 1)


def product_kernel(col_block, info_ref, c_ref, rows_ref, out_ref):
    row_block, width = out_ref.shape
    half = width // 2

    @pl.when(pl.program_id(0) == 0)
    def _():
        out_ref[...] = jnp.zeros_like(out_ref)

    c = c_ref[...]
    r = rows_ref[...].astype(jnp.float32)
    a = c * r
    b = c * pltpu.roll(r, half, 1)
    low = lax.broadcasted_iota(jnp.int32, c.shape, 1) < half
    product = jnp.where(low, a - pltpu.roll(a, half, 1), b + pltpu.roll(b, half, 1))
    high = product.astype(jnp.bfloat16)
    rest = (product - high.astype(jnp.float32)).astype(jnp.bfloat16)
    values = jnp.concatenate([high, rest], axis=1)
    sums = jnp.dot(
        pick_rows(info_ref[0], row_block, col_block), values, preferred_element_type=jnp.float32
    )
    out_ref[...] += sums[:, :width] + sums[:, width:]


def segment(kernel, name, info, arrays, row_block, col_block):
    total, width = arrays[0].shape
    chunk = min(1024, total)
    steps = total // chunk
    return pl.pallas_call(
        functools.partial(kernel, col_block),
        out_shape=jax.ShapeDtypeStruct((row_block, width), jnp.float32),
        grid=(steps,),
        in_specs=[pl.BlockSpec((1, 1, chunk), lambda i: (i, 0, 0))]
        + [pl.BlockSpec((chunk, width), lambda i: (i, 0))] * len(arrays),
        out_specs=pl.BlockSpec((row_block, width), lambda i: (0, 0)),
        cost_estimate=pl.CostEstimate(
            flops=2 * row_block * total * 2 * width,
            bytes_accessed=total * width * 4,
            transcendentals=0,
        ),
        name=name,
    )(info.reshape(steps, 1, chunk), *arrays)


def collect_kernel(
    count, num_ref, den_ref, out_ref, num_held, den_held, num_send, num_recv, den_send, den_recv
):
    me = lax.axis_index("acol")
    barrier = pltpu.get_barrier_semaphore()
    for step in range(1, count):
        pl.semaphore_signal(
            barrier,
            inc=1,
            device_id=(lax.axis_index("arow"), lax.rem(me + step, count)),
            device_id_type=MESH,
        )
    pl.semaphore_wait(barrier, count - 1)

    def copies(to, slot):
        return [
            pltpu.make_async_remote_copy(
                src_ref=part.at[to],
                dst_ref=held.at[slot],
                send_sem=send.at[to],
                recv_sem=recv.at[slot],
                device_id=(lax.axis_index("arow"), to),
                device_id_type=MESH,
            )
            for part, held, send, recv in (
                (den_ref, den_held, den_send, den_recv),
                (num_ref, num_held, num_send, num_recv),
            )
        ]

    for step in range(1, count):
        for copy in copies(lax.rem(me + step, count), me):
            copy.start()
    num = num_ref[me]
    den = den_ref[me]
    for step in range(1, count):
        other = lax.rem(me + step, count)
        for copy in copies(other, other):
            copy.wait()
        num = num + num_held[other]
        den = den + den_held[other]
    out_ref[...] = num / (den + RIDGE)


def collect(numerator, denominator, count):
    rows, width = numerator.shape
    share_rows = rows // count
    shape = (count, share_rows, width)
    return pl.pallas_call(
        functools.partial(collect_kernel, count),
        out_shape=jax.ShapeDtypeStruct((share_rows, width), jnp.float32),
        in_specs=[pl.BlockSpec(memory_space=pltpu.VMEM)] * 2,
        out_specs=pl.BlockSpec(memory_space=pltpu.VMEM),
        scratch_shapes=[pltpu.VMEM(shape, jnp.float32)] * 2
        + [pltpu.SemaphoreType.DMA((count,))] * 4,
        compiler_params=pltpu.CompilerParams(collective_id=1, has_side_effects=True),
        name="collect",
    )(numerator.reshape(shape), denominator.reshape(shape))


def split_parts(values, count):
    parts = []
    for _ in range(count - 1):
        high = values.astype(jnp.bfloat16)
        parts.append(high)
        values = values - high.astype(jnp.float32)
    parts.append(values.astype(jnp.bfloat16))
    return parts


def one_hot(found):
    return jnp.where(found, 1.0, 0.0).astype(jnp.bfloat16)


def contract(left, right, left_dim, right_dim):
    return lax.dot_general(
        left, right, (((left_dim,), (right_dim,)), ((), ())), preferred_element_type=jnp.float32
    )


def stream_kernel(
    row_count, col_count, near, lanes, chunk, fold,
    rows_ref, base_ref, gain_ref, pair_ref, weight_ref, model_ref,
    out_ref, flag_ref,
    model, rows_v, send_rows, send_labels, rank_ref, pos_ref, rows_in, name_in, label_v, label_s,
    table_v, table_s, first_ref, second_ref,
    column_ref, gain_parts, gain_rows, picked, c_table, c_rows, lookup, firsts, weights, sums,
    parts, half_in, halves, final_in,
    base_send, base_recv, name_send, name_recv, over_send, over_recv,
    half_send, half_recv, final_send, final_recv, gain_send, gain_recv, local_sem,
):
    devices = row_count * col_count
    count, width = rows_ref.shape
    half = width // 2
    blocks = count // LANES
    far = lanes - near
    table_rows = weight_ref.shape[0]
    slots = table_rows * LANES
    slot_bits = slots.bit_length() - 1
    row_block = sums.shape[0]
    col_block = gain_parts.shape[0]
    share_rows = gain_ref.shape[0]
    pairs = col_count // 2
    my_row = lax.axis_index("arow")
    my_col = lax.axis_index("acol")
    me = my_row * col_count + my_col
    parity = lax.rem(my_col, 2)
    my_pair = my_col // 2
    partner = my_col + 1 - 2 * parity
    aside = (my_row, partner)
    barrier = pltpu.get_barrier_semaphore()

    def place(index):
        return (index // col_count, lax.rem(index, col_count))

    def remote(src, dst, send, recv, to):
        return pltpu.make_async_remote_copy(
            src_ref=src, dst_ref=dst, send_sem=send, recv_sem=recv,
            device_id=to, device_id_type=MESH,
        )

    bring = pltpu.make_async_copy(rows_ref, rows_v, local_sem.at[1])
    bring.start()
    load = pltpu.make_async_copy(model_ref, model, local_sem.at[0])
    load.start()

    def greet(step, carry):
        pl.semaphore_signal(
            barrier, inc=1, device_id=place(lax.rem(me + step, devices)), device_id_type=MESH
        )
        return carry

    lax.fori_loop(1, devices, greet, 0)
    for line in range(table_rows):
        first_ref[line : line + 1, :] = jnp.clip(
            pair_ref[line, 0:1, :] - my_row * row_block, 0, row_block - 1
        )
        second_ref[line : line + 1, :] = jnp.clip(
            pair_ref[line, 1:2, :] - my_col * col_block, 0, col_block - 1
        )
    table_v[...] = first_ref[...] * (col_block // 2) + (second_ref[...] >> 1)

    upper = one_hot(
        lax.broadcasted_iota(jnp.int32, (LANES, LANES), 0)
        < lax.broadcasted_iota(jnp.int32, (LANES, LANES), 1)
    )
    tile = lax.broadcasted_iota(jnp.int32, (devices, LANES), 0)
    before = jnp.zeros((devices, 1), jnp.float32)
    for block in range(blocks):
        hit = tile == base_ref[block : block + 1, :] >> slot_bits
        hits = jnp.where(hit, 1.0, 0.0)
        within = jnp.dot(hits.astype(jnp.bfloat16), upper, preferred_element_type=jnp.float32)
        ranking = jnp.sum(jnp.where(hit, within + before, 0.0), axis=0, keepdims=True)
        before = before + jnp.sum(hits, axis=1, keepdims=True)
        rank_ref[block : block + 1, :] = ranking.astype(jnp.int32)
    ranks = rank_ref[...]
    over = ranks >= near
    overs = one_hot(over)
    lower = one_hot(
        lax.broadcasted_iota(jnp.int32, (blocks, blocks), 0)
        > lax.broadcasted_iota(jnp.int32, (blocks, blocks), 1)
    )
    earlier = jnp.dot(lower, overs, preferred_element_type=jnp.float32)
    over_rank = jnp.dot(overs, upper, preferred_element_type=jnp.float32) + jnp.sum(
        earlier, axis=1, keepdims=True
    )
    over_spot = near + over_rank.astype(jnp.int32)
    lost = jnp.max(jnp.where(over & (over_spot >= lanes), 1.0, 0.0), axis=(0, 1), keepdims=True)
    over_at = jnp.where(over, over_spot, -1)
    pos_ref[...] = jnp.where(
        over,
        jnp.where(over_spot < lanes, devices * near + over_spot - near, -1),
        (base_ref[...] >> slot_bits) * near + ranks,
    )

    spots = lax.broadcasted_iota(jnp.int32, (LANES, LANES), 0)
    over_spots = lax.broadcasted_iota(jnp.int32, (lanes, LANES), 0)
    sub = lax.broadcasted_iota(jnp.int32, (8, LANES), 0)
    names = jnp.zeros((3 * devices, LANES), jnp.float32)
    marks = jnp.zeros((8, lanes), jnp.float32)
    for block in range(blocks):
        slot = base_ref[block : block + 1, :]
        owner = slot >> slot_bits
        high = ((slot & (slots - 1)) >> 6).astype(jnp.float32)
        low_bits = (slot & 63).astype(jnp.float32)
        hit = tile == owner
        pieces = jnp.concatenate(
            [jnp.where(hit, high, 0.0), jnp.where(hit, low_bits, 0.0), jnp.where(hit, 1.0, 0.0)],
            axis=0,
        ).astype(jnp.bfloat16)
        names = names + contract(pieces, one_hot(spots == ranks[block : block + 1, :]), 1, 1)
        whole = jnp.where(
            sub == 0,
            owner.astype(jnp.float32),
            jnp.where(sub == 1, high, jnp.where(sub == 2, low_bits, jnp.where(sub == 3, 1.0, 0.0))),
        ).astype(jnp.bfloat16)
        marks = marks + contract(
            whole, one_hot(over_spots == over_at[block : block + 1, :]), 1, 1
        )
    lane = lax.broadcasted_iota(jnp.int32, (devices, LANES), 1)
    label = names[:devices] * 64.0 + names[devices : 2 * devices]
    label = jnp.where(names[2 * devices :] > 0.5, label, float(slots))
    label = jnp.where(lane == LANES - 1, lost, label).astype(jnp.int32)
    mark = marks[0:1] * float(slots) + marks[1:2] * 64.0 + marks[2:3]
    mark = jnp.where(marks[3:4] > 0.5, mark, -1.0).astype(jnp.int32)
    for index in range(devices):
        send_labels[index] = jnp.concatenate([label[index : index + 1, :], mark], axis=1)
    name_in[me] = send_labels[me]

    pl.semaphore_wait(barrier, devices - 1)

    def name_copy(to, slot):
        return remote(
            send_labels.at[to], name_in.at[slot], name_send, name_recv, place(to)
        )

    def base_copy(to, slot):
        return remote(
            send_rows.at[to], rows_in.at[slot, pl.ds(0, near)],
            base_send, base_recv, place(to),
        )

    def over_copy(sources, to, stage):
        there = rows_in.at[sources, pl.ds(near, far)]
        return remote(there, there, over_send, over_recv.at[stage], to)

    def along(step):
        return over_copy(me, (lax.rem(my_row + step, row_count), my_col), 0)

    def across(source_row, step):
        to = (my_row, lax.rem(my_col + 2 * step, col_count))
        return over_copy(source_row * col_count + my_col, to, 1)

    def relay(source):
        return over_copy(source, (my_row, partner), 2)

    column = me // row_count
    part = lax.rem(me, row_count)

    def gain_copy(row, col, slot):
        return remote(
            gain_ref, column_ref.at[slot], gain_send.at[row], gain_recv.at[slot], (row, col)
        )

    for row in range(row_count):
        stays = jnp.logical_and(row == my_row, column == my_col)

        @pl.when(jnp.logical_not(stays))
        def _():
            gain_copy(row, column, part).start()

        @pl.when(stays)
        def _():
            column_ref[part] = gain_ref[...]

    def send_names(step, carry):
        name_copy(lax.rem(me + step, devices), me).start()
        return carry

    lax.fori_loop(1, devices, send_names, 0)

    def arrange(first, size):
        at = lax.broadcasted_iota(jnp.int32, (size, LANES), 0) + first
        hot = jnp.concatenate(
            [one_hot(at == pos_ref[block : block + 1, :]) for block in range(blocks)], axis=1
        )
        return jnp.dot(hot, rows_v[...], preferred_element_type=jnp.float32).astype(jnp.bfloat16)

    bring.wait()
    rows_in[me, near:, :] = arrange(devices * near, far)
    for step in range(1, row_count):
        along(step).start()
    for step in range(1, pairs):
        across(my_row, step).start()
    relay(me).start()


    groups = devices // fold

    def arrange_tiles(step, carry):
        group = lax.rem(step + (my_row + 1) * (col_count // fold), groups)
        got = arrange(group * (fold * near), fold * near)
        send_rows[pl.ds(group * fold, fold)] = got.reshape(fold, near, width)

        @pl.when(step < groups - col_count // fold)
        def _():
            for number in range(fold):
                base_copy(group * fold + number, me).start()

        return carry

    lax.fori_loop(0, groups, arrange_tiles, 0)
    rows_in[me, :near, :] = send_rows[me]

    for slot in range(row_count):
        source = my_col * row_count + slot

        @pl.when(source != me)
        def _():
            gain_copy(0, my_col, slot).wait_recv()

    gains = split_parts(column_ref[...].reshape(col_block, width), 3)
    for number in range(3):
        gain_parts[:, number * width : (number + 1) * width] = gains[number]
    gain_parts[:, 3 * width :] = one_hot(
        (lax.broadcasted_iota(jnp.int32, (col_block, width), 0) & 1) == 1
    )
    seconds = lax.broadcasted_iota(jnp.int32, (col_block, LANES), 0)

    def spread_gains(number, carry):
        hot = jnp.concatenate(
            [
                one_hot(seconds == second_ref[pl.ds(number * (chunk // LANES) + k, 1), :])
                for k in range(chunk // LANES)
            ],
            axis=1,
        )
        got = contract(hot, gain_parts[...], 0, 0)
        at = pl.ds(pl.multiple_of(number * chunk, chunk), chunk)
        gain_rows[at, :width] = (got[:, :width] + got[:, width : 2 * width]) + got[
            :, 2 * width : 3 * width
        ]
        gain_rows[at, width:] = got[:, 3 * width :]
        return carry

    lax.fori_loop(0, slots // chunk, spread_gains, 0)
    to_table = pltpu.make_async_copy(table_v, table_s, local_sem.at[2])
    to_table.start()
    to_table.wait()
    lookup[:table_rows, :] = (first_ref[...] >> 1).astype(jnp.float32).astype(jnp.bfloat16)
    lookup[table_rows:, :] = (
        (((first_ref[...] & 1) << WEIGHT_BITS) + weight_ref[...]).astype(jnp.float32)
    ).astype(jnp.bfloat16)

    remote(
        send_labels.at[pl.ds(0, devices - 1)], name_in.at[pl.ds(0, devices - 1)],
        name_send, name_recv, aside,
    ).wait()
    lane = lax.broadcasted_iota(jnp.int32, name_in.shape, 2)
    flag_ref[0, 0] = jnp.max(jnp.where(lane == LANES - 1, name_in[...], 0).astype(jnp.float32)).astype(
        jnp.int32
    )
    lane = lax.broadcasted_iota(jnp.int32, (1, LANES), 1)
    batch = fold * lanes

    def name_rows(step, carry):
        labels = []
        for number in range(fold):
            source = step * fold + number
            there = name_in[source][:, LANES:] - me * slots
            there = jnp.where((there >= 0) & (there < slots), there, slots)
            near_part = jnp.where(lane < near, name_in[source][:, :LANES], there[:, :LANES])
            if lanes > LANES:
                near_part = jnp.concatenate([near_part, there[:, LANES:]], axis=1)
            near_part = jnp.clip(near_part, 0, slots)
            for line in range(lanes // LANES):
                label_v[source * (lanes // LANES) + line] = near_part[
                    :, line * LANES : (line + 1) * LANES
                ]
            labels.append(near_part)
        label = jnp.concatenate(labels, axis=1)
        hot = one_hot(lax.broadcasted_iota(jnp.int32, (LANES, batch), 0) == (label & (LANES - 1)))
        found = jnp.dot(lookup[...], hot, preferred_element_type=jnp.float32)
        line = lax.broadcasted_iota(jnp.int32, (table_rows, batch), 0) == label >> 7
        upper_bits = jnp.sum(
            jnp.where(line, found[:table_rows], 0.0), axis=0, keepdims=True
        ).astype(jnp.int32)
        rest = jnp.sum(
            jnp.where(line, found[table_rows:], 0.0), axis=0, keepdims=True
        ).astype(jnp.int32)
        firsts[step] = 2 * upper_bits + (rest >> WEIGHT_BITS)
        weights[step] = (rest & ((1 << WEIGHT_BITS) - 1)).astype(jnp.float32)
        return carry

    lax.fori_loop(0, devices // fold, name_rows, 0)
    to_scalar = pltpu.make_async_copy(label_v, label_s, local_sem.at[1])
    to_scalar.start()

    over_copy(pl.ds(0, row_count - 1), aside, 0).wait_recv()
    for step in range(1, row_count):
        source_row = lax.rem(my_row + step, row_count)
        for other in range(1, pairs):
            across(source_row, other).start()
        relay(source_row * col_count + my_col).start()

    def send_plane(step, carry):
        base_copy(my_row * col_count + lax.rem(my_col + step, col_count), me).start()
        return carry

    lax.fori_loop(1, col_count, send_plane, 0)

    load.wait()
    low = lax.broadcasted_iota(jnp.int32, (chunk, width), 1) < half
    c_table[slots:, :] = jnp.zeros((c_table.shape[0] - slots, width), jnp.float32)

    def piece(number, carry):
        begin = number * chunk

        def fetch(line, carry):
            to = pl.multiple_of(line * 2 * LANES, 2 * LANES)
            window = table_s.at[number * (chunk // LANES) + line]
            for at in range(0, LANES, GROUP):
                held = [model[window[at + k]].astype(jnp.float32) for k in range(GROUP)]
                for k in range(GROUP):
                    picked[pl.ds(to + 2 * (at + k), 2), :] = held[k]
            return carry

        lax.fori_loop(0, chunk // LANES, fetch, 0)
        at = pl.ds(pl.multiple_of(begin, chunk), chunk)
        m = jnp.where(
            gain_rows[at, width:] > 0.5,
            picked[pl.ds(1, chunk, stride=2), :],
            picked[pl.ds(0, chunk, stride=2), :],
        )
        g = gain_rows[at, :width]
        a = m * g
        b = m * pltpu.roll(g, half, 1)
        c_table[at, :] = jnp.where(
            low, a + pltpu.roll(a, half, 1), pltpu.roll(b, half, 1) - b
        )
        return carry

    lax.fori_loop(0, slots // chunk, piece, 0)

    to_scalar.wait()

    def grab(line, carry):
        to = pl.multiple_of(line * LANES, LANES)
        window = label_s.at[line, 0]
        for at in range(0, LANES, GROUP):
            held = [c_table[pl.ds(window[at + k], 1), :] for k in range(GROUP)]
            for k in range(GROUP):
                c_rows[pl.ds(to + at + k, 1), :] = held[k]
        return carry

    middle = devices * lanes // LANES // 2
    lax.fori_loop(0, middle, grab, 0)
    over_copy(pl.ds(0, row_count * (pairs - 1)), aside, 1).wait_recv()
    for step in range(1, pairs):
        for source_row in range(row_count):
            source = source_row * col_count + lax.rem(my_col + 2 * step, col_count)
            over_copy(source, aside, 2).start()

    lax.fori_loop(middle, 2 * middle, grab, 0)
    low = lax.broadcasted_iota(jnp.int32, (batch, width), 1) < half
    sums[...] = jnp.zeros_like(sums)

    remote(
        send_rows.at[pl.ds(0, devices - 1)], rows_in.at[pl.ds(0, devices - 1), pl.ds(0, near)],
        base_send, base_recv, aside,
    ).wait()
    over_copy(pl.ds(0, row_count * pairs), aside, 2).wait_recv()

    def add_product(step, carry):
        c = c_rows[pl.ds(pl.multiple_of(step * batch, batch), batch), :]
        r = rows_in[pl.ds(step * fold, fold)].reshape(batch, width).astype(jnp.float32)
        turned = pltpu.roll(c, half, 1)
        product = jnp.where(low, c, turned) * r + jnp.where(low, -turned, c) * pltpu.roll(
            r, half, 1
        )
        power = c * c
        power = power + pltpu.roll(power, half, 1)
        power_high = power.astype(jnp.bfloat16).astype(jnp.float32)
        power = jnp.where(low, power_high, power - power_high).astype(jnp.bfloat16)
        values = jnp.concatenate(split_parts(product, 2) + [power], axis=1)
        pick = jnp.where(
            lax.broadcasted_iota(jnp.int32, (row_block, batch), 0) == firsts[step],
            weights[step],
            0.0,
        ).astype(jnp.bfloat16)
        sums[...] += jnp.dot(pick, values, preferred_element_type=jnp.float32)
        return carry

    lax.fori_loop(0, devices // fold, add_product, 0)

    numerator = sums[:, :width] + sums[:, width : 2 * width]
    denominator = sums[:, 2 * width :]
    denominator = denominator + pltpu.roll(denominator, half, 1)
    side = share_rows // 2
    low = lax.broadcasted_iota(jnp.int32, (side, width), 1) < half
    for col in range(col_count):
        at = col * share_rows
        parts[col % 2, col // 2, :share_rows, :] = numerator[at : at + share_rows]
        parts[col % 2, col // 2, share_rows:, :] = jnp.where(
            low, denominator[at : at + side], denominator[at + side : at + share_rows]
        )
    swap = remote(
        parts.at[1 - parity], half_in, half_send, half_recv, (my_row, partner)
    )
    swap.start()

    over_copy(pl.ds(0, devices - 1), aside, 0).wait_send()
    for row in range(row_count):
        stays = jnp.logical_and(row == my_row, column == my_col)

        @pl.when(jnp.logical_not(stays))
        def _():
            gain_copy(row, column, part).wait_send()

    swap.wait()
    halves[...] = parts[parity] + half_in[...]

    def final_copy(to, slot, device):
        return remote(halves.at[to], final_in.at[slot], final_send, final_recv, device)

    for step in range(1, pairs):
        to = lax.rem(my_pair + step, pairs)
        final_copy(to, my_pair, (my_row, 2 * to + parity)).start()
    final_copy(pl.ds(0, pairs - 1), pl.ds(0, pairs - 1), aside).wait()
    total = halves[my_pair]
    for step in range(1, pairs):
        total = total + final_in[lax.rem(my_pair + step, pairs)]
    held = total[share_rows:]
    turned = pltpu.roll(held, half, 1)
    out_ref[:side, :] = total[:side] / (jnp.where(low, held, turned) + RIDGE)
    out_ref[side:, :] = total[side:share_rows] / (jnp.where(low, turned, held) + RIDGE)


def stream(rows, baseline, gains, pair_table, weight, model_vis, row_count, col_count):
    devices = row_count * col_count
    count, width = rows.shape
    row_block, col_block, _ = model_vis.shape
    slots = weight.shape[0]
    share_rows = gains.shape[0]
    mean = count // devices
    capacity = 4 * mean
    lanes = -(-capacity // LANES) * LANES
    near = -(-3 * mean // 32) * 16
    far = lanes - near
    blocks = count // LANES
    pairs = row_block * col_block // 2
    total = devices * lanes
    chunk = min(512, slots)
    fold = 4
    half_count = col_count // 2
    piece = (half_count, share_rows + share_rows // 2, width)
    vmem = pl.BlockSpec(memory_space=pltpu.VMEM)
    dma = pltpu.SemaphoreType.DMA
    return pl.pallas_call(
        functools.partial(stream_kernel, row_count, col_count, near, lanes, chunk, fold),
        out_shape=(
            jax.ShapeDtypeStruct(gains.shape, jnp.float32),
            jax.ShapeDtypeStruct((1, 1), jnp.int32),
        ),
        in_specs=[pl.BlockSpec(memory_space=pl.ANY)]
        + [vmem] * 4
        + [pl.BlockSpec(memory_space=pl.ANY)],
        out_specs=(vmem, pl.BlockSpec(memory_space=pltpu.SMEM)),
        scratch_shapes=[
            pltpu.VMEM((pairs, 2, width), jnp.bfloat16),
            pltpu.VMEM((count, width), jnp.bfloat16),
            pltpu.VMEM((devices, near, width), jnp.bfloat16),
            pltpu.VMEM((devices, 1, LANES + lanes), jnp.int32),
            pltpu.VMEM((blocks, LANES), jnp.int32),
            pltpu.VMEM((blocks, LANES), jnp.int32),
            pltpu.VMEM((devices, lanes, width), jnp.bfloat16),
            pltpu.VMEM((devices, 1, LANES + lanes), jnp.int32),
            pltpu.VMEM((total // LANES, 1, LANES), jnp.int32),
            pltpu.SMEM((total // LANES, 1, LANES), jnp.int32),
            pltpu.VMEM((slots // LANES, LANES), jnp.int32),
            pltpu.SMEM((slots // LANES, LANES), jnp.int32),
            pltpu.VMEM((slots // LANES, LANES), jnp.int32),
            pltpu.VMEM((slots // LANES, LANES), jnp.int32),
            pltpu.VMEM((row_count, share_rows, width), jnp.float32),
            pltpu.VMEM((col_block, 4 * width), jnp.bfloat16),
            pltpu.VMEM((slots, 2 * width), jnp.float32),
            pltpu.VMEM((2 * chunk, width), jnp.float32),
            pltpu.VMEM((slots + 8, width), jnp.float32),
            pltpu.VMEM((total, width), jnp.float32),
            pltpu.VMEM((2 * slots // LANES, LANES), jnp.bfloat16),
            pltpu.VMEM((devices // fold, 1, fold * lanes), jnp.int32),
            pltpu.VMEM((devices // fold, 1, fold * lanes), jnp.float32),
            pltpu.VMEM((row_block, 3 * width), jnp.float32),
            pltpu.VMEM((2,) + piece, jnp.float32),
            pltpu.VMEM(piece, jnp.float32),
            pltpu.VMEM(piece, jnp.float32),
            pltpu.VMEM(piece, jnp.float32),
        ]
        + [dma] * 5
        + [dma((3,))]
        + [dma] * 4
        + [dma((row_count,))] * 2
        + [dma((3,))],
        compiler_params=pltpu.CompilerParams(
            collective_id=2, has_side_effects=True, vmem_limit_bytes=63 << 20
        ),
        name="stream",
    )(
        rows,
        baseline.reshape(blocks, LANES),
        gains,
        pair_table.reshape(slots // LANES, LANES, 2).transpose(0, 2, 1),
        weight.reshape(slots // LANES, LANES),
        model_vis.reshape(pairs, 2, width),
    )


def padded(row_count, col_count, row_data, row_baseline, pair_table, lengths, model_vis, gains):
    devices = row_count * col_count
    slots = lengths.shape[0]
    capacity = 4 * row_data.shape[0] // devices
    row_block, col_block, width = model_vis.shape
    total = devices * capacity
    my_row = lax.axis_index("arow")
    my_col = lax.axis_index("acol")
    first = pair_table[:, 0] - my_row * row_block
    second = pair_table[:, 1] - my_col * col_block
    pair = first * (col_block // 2) + second // 2
    table = ((pair << WEIGHT_BITS) + lengths) * (2 * col_block) + 2 * second
    table = jnp.concatenate([table, jnp.zeros((LANES,), jnp.int32)])
    outgoing, labels = route(row_data, row_baseline, devices, capacity, slots)
    names, column_gains = share(
        labels.reshape(devices, 1, capacity), gains, row_count, col_count
    )
    outgoing, names = lax.optimization_barrier((outgoing, names))
    arrived = lax.all_to_all(
        outgoing.reshape(devices, capacity, width),
        ("arow", "acol"),
        split_axis=0,
        concat_axis=0,
        tiled=True,
    ).reshape(total, width)
    c, info = gather(
        names.reshape(total), table, model_vis, column_gains.reshape(col_block, width)
    )
    power = segment(power_kernel, "power", info, [c], row_block, col_block)
    product = segment(product_kernel, "product", info, [c, arrived], row_block, col_block)
    return collect(product, power, col_count)


def local(row_count, col_count, row_data, row_baseline, pair_table, lengths, model_vis, gains):
    updated, flag = stream(
        row_data, row_baseline, gains, pair_table, lengths, model_vis, row_count, col_count
    )
    return lax.cond(
        flag[0, 0] > 0,
        lambda: padded(
            row_count, col_count, row_data, row_baseline, pair_table, lengths, model_vis, gains
        ),
        lambda: updated,
    )


def solution(mesh):
    placed = (
        P(("arow", "acol"), None),
        P(("arow", "acol")),
        P(("arow", "acol"), None),
        P(("arow", "acol")),
        P("arow", "acol", None),
        P(("arow", "acol"), None),
    )
    return jax.shard_map(
        functools.partial(local, mesh.shape["arow"], mesh.shape["acol"]),
        mesh=mesh,
        in_specs=placed,
        out_specs=P(("arow", "acol"), None),
        check_vma=False,
    )
```

```python
import functools

import jax
import jax.numpy as jnp
from jax import lax
from jax.experimental import pallas as pl
from jax.experimental.pallas import tpu as pltpu
from jax.sharding import PartitionSpec as P

RIDGE = 1.0
LANES = 128
GROUP = 32
WEIGHT_BITS = 4
MESH = pl.DeviceIdType.MESH


def rows_at(ref, start, count):
    return ref[pl.ds(start, count), :]


def route_kernel(
    devices, capacity, slots, rows_ref, base_ref, out_ref, label_ref,
    wide, spread, target, local_id, empty, target_s, local_s, sems,
):
    blocks = base_ref.shape[0]
    count = rows_ref.shape[0]
    empty[...] = jnp.full(empty.shape, slots, jnp.int32)
    fill = pltpu.make_async_copy(empty, label_ref, sems.at[0])
    fill.start()
    order = lax.broadcasted_iota(jnp.int32, (LANES, LANES), 0)
    upper = (order < lax.broadcasted_iota(jnp.int32, (LANES, LANES), 1)).astype(jnp.bfloat16)
    tile = lax.broadcasted_iota(jnp.int32, (devices, LANES), 0)
    before = jnp.zeros((devices, 1), jnp.float32)
    for block in range(blocks):
        slot = base_ref[block : block + 1, :]
        owner = slot // slots
        hit = tile == owner
        hits = jnp.where(hit, 1.0, 0.0)
        within = jnp.dot(hits.astype(jnp.bfloat16), upper, preferred_element_type=jnp.float32)
        ranking = jnp.sum(jnp.where(hit, within + before, 0.0), axis=0, keepdims=True)
        before = before + jnp.sum(hits, axis=1, keepdims=True)
        target[block : block + 1, :] = owner * capacity + ranking.astype(jnp.int32)
        local_id[block : block + 1, :] = slot - owner * slots
    to_target = pltpu.make_async_copy(target, target_s, sems.at[1])
    to_target.start()
    to_local = pltpu.make_async_copy(local_id, local_s, sems.at[2])
    to_local.start()
    wide[...] = rows_ref[...].astype(jnp.float32)
    spread[...] = jnp.zeros_like(spread)
    to_target.wait()
    to_local.wait()
    fill.wait()

    def place_block(block, carry):
        def place(group, carry):
            first = group * GROUP
            spots = [target_s[block, first + k] for k in range(GROUP)]
            ids = [local_s[block, first + k] for k in range(GROUP)]
            held = [
                wide[pl.ds(block * LANES + first + k, 1), :] for k in range(GROUP)
            ]
            for k in range(GROUP):
                label_ref[spots[k]] = ids[k]
                spread[pl.ds(spots[k], 1), :] = held[k]
            return carry

        return lax.fori_loop(0, LANES // GROUP, place, carry)

    lax.fori_loop(0, count // LANES, place_block, 0)
    out_ref[...] = spread[...].astype(jnp.bfloat16)


def route(rows, baseline, devices, capacity, slots):
    count, width = rows.shape
    blocks = count // LANES
    total = devices * capacity
    return pl.pallas_call(
        functools.partial(route_kernel, devices, capacity, slots),
        out_shape=(
            jax.ShapeDtypeStruct((total, width), jnp.bfloat16),
            jax.ShapeDtypeStruct((total,), jnp.int32),
        ),
        in_specs=[pl.BlockSpec(memory_space=pltpu.VMEM)] * 2,
        out_specs=(
            pl.BlockSpec(memory_space=pltpu.VMEM),
            pl.BlockSpec(memory_space=pltpu.SMEM),
        ),
        scratch_shapes=[
            pltpu.VMEM((count, width), jnp.float32),
            pltpu.VMEM((total, width), jnp.float32),
            pltpu.VMEM((blocks, LANES), jnp.int32),
            pltpu.VMEM((blocks, LANES), jnp.int32),
            pltpu.VMEM((total,), jnp.int32),
            pltpu.SMEM((blocks, LANES), jnp.int32),
            pltpu.SMEM((blocks, LANES), jnp.int32),
            pltpu.SemaphoreType.DMA((3,)),
        ],
        name="route",
    )(rows, baseline.reshape(blocks, LANES))


def share_kernel(
    row_count, col_count, label_ref, gain_ref, name_ref, column_ref,
    send_sem, recv_sem, gain_send, gain_recv, local_sem,
):
    devices = row_count * col_count
    my_row = lax.axis_index("arow")
    my_col = lax.axis_index("acol")
    me = my_row * col_count + my_col
    barrier = pltpu.get_barrier_semaphore()

    def place(index):
        return (index // col_count, lax.rem(index, col_count))

    def greet(step, carry):
        pl.semaphore_signal(
            barrier, inc=1, device_id=place(lax.rem(me + step, devices)), device_id_type=MESH
        )
        return carry

    lax.fori_loop(1, devices, greet, 0)
    own = pltpu.make_async_copy(label_ref.at[me], name_ref.at[me], local_sem.at[0])
    own.start()
    pl.semaphore_wait(barrier, devices - 1)

    def label_copy(to, slot):
        return pltpu.make_async_remote_copy(
            src_ref=label_ref.at[to],
            dst_ref=name_ref.at[slot],
            send_sem=send_sem.at[to],
            recv_sem=recv_sem.at[slot],
            device_id=place(to),
            device_id_type=MESH,
        )

    def send(step, carry):
        label_copy(lax.rem(me + step, devices), me).start()
        return carry

    lax.fori_loop(1, devices, send, 0)
    column = me // row_count
    part = lax.rem(me, row_count)

    def gain_copy(row, col, slot):
        return pltpu.make_async_remote_copy(
            src_ref=gain_ref,
            dst_ref=column_ref.at[slot],
            send_sem=gain_send.at[row],
            recv_sem=gain_recv.at[slot],
            device_id=(row, col),
            device_id_type=MESH,
        )

    own_gain = pltpu.make_async_copy(gain_ref, column_ref.at[part], local_sem.at[1])
    for row in range(row_count):
        stays = jnp.logical_and(row == my_row, column == my_col)

        @pl.when(jnp.logical_not(stays))
        def _():
            gain_copy(row, column, part).start()

        @pl.when(stays)
        def _():
            own_gain.start()

    for row in range(row_count):
        stays = jnp.logical_and(row == my_row, column == my_col)

        @pl.when(jnp.logical_not(stays))
        def _():
            gain_copy(row, column, part).wait_send()

        @pl.when(stays)
        def _():
            own_gain.wait()

    for slot in range(row_count):
        source = my_col * row_count + slot

        @pl.when(source != me)
        def _():
            gain_copy(0, my_col, slot).wait_recv()

    def finish(step, carry):
        other = lax.rem(me + step, devices)
        label_copy(other, other).wait()
        return carry

    lax.fori_loop(1, devices, finish, 0)
    own.wait()


def share(labels, gains, row_count, col_count):
    devices = row_count * col_count
    return pl.pallas_call(
        functools.partial(share_kernel, row_count, col_count),
        out_shape=(
            jax.ShapeDtypeStruct(labels.shape, jnp.int32),
            jax.ShapeDtypeStruct((row_count,) + gains.shape, jnp.float32),
        ),
        in_specs=[pl.BlockSpec(memory_space=pltpu.VMEM)] * 2,
        out_specs=(pl.BlockSpec(memory_space=pltpu.VMEM),) * 2,
        scratch_shapes=[
            pltpu.SemaphoreType.DMA((devices,)),
            pltpu.SemaphoreType.DMA((devices,)),
            pltpu.SemaphoreType.DMA((row_count,)),
            pltpu.SemaphoreType.DMA((row_count,)),
            pltpu.SemaphoreType.DMA((2,)),
        ],
        compiler_params=pltpu.CompilerParams(collective_id=0, has_side_effects=True),
        name="share",
    )(labels, gains)


def gather_kernel(
    col_block, chunk, name_ref, table_ref, model_ref, gain_ref, c_ref, info_ref,
    model, pair_gain, gain_rows, picked, sem,
):
    total = c_ref.shape[0]
    width = c_ref.shape[1]
    half = width // 2
    load = pltpu.make_async_copy(model_ref, model, sem)
    load.start()
    shift = col_block.bit_length() + WEIGHT_BITS
    odd = lax.broadcasted_iota(jnp.int32, gain_ref.shape, 0) & 1
    pair_gain[pl.ds(0, col_block, stride=2), :] = jnp.where(odd == 0, gain_ref[...], 0.0)
    pair_gain[pl.ds(1, col_block, stride=2), :] = jnp.where(odd == 1, gain_ref[...], 0.0)

    def look(group, carry):
        first = group * GROUP
        names = [name_ref[first + k] for k in range(GROUP)]
        infos = [table_ref[name] for name in names]
        held = [pair_gain[pl.ds(info & (2 * col_block - 1), 2), :] for info in infos]
        for k in range(GROUP):
            info_ref[first + k] = infos[k]
            gain_rows[pl.ds(2 * (first + k), 2), :] = held[k]
        return carry

    lax.fori_loop(0, total // GROUP, look, 0)
    load.wait()

    def piece(number, carry):
        start = number * chunk

        def fetch(group, carry):
            first = group * GROUP
            infos = [info_ref[start + first + k] for k in range(GROUP)]
            held = [model[info >> shift].astype(jnp.float32) for info in infos]
            for k in range(GROUP):
                picked[pl.ds(2 * (first + k), 2), :] = held[k]
            return carry

        lax.fori_loop(0, chunk // GROUP, fetch, 0)
        at = pl.multiple_of(2 * start, 2 * chunk)
        m_even = picked[pl.ds(0, chunk, stride=2), :]
        m_odd = picked[pl.ds(1, chunk, stride=2), :]
        g_even = gain_rows[pl.ds(at, chunk, stride=2), :]
        g_odd = gain_rows[pl.ds(at + 1, chunk, stride=2), :]
        a = m_even * g_even + m_odd * g_odd
        b = m_even * pltpu.roll(g_even, half, 1) + m_odd * pltpu.roll(g_odd, half, 1)
        low = lax.broadcasted_iota(jnp.int32, (chunk, width), 1) < half
        c_ref[pl.ds(pl.multiple_of(start, chunk), chunk), :] = jnp.where(
            low, a + pltpu.roll(a, half, 1), pltpu.roll(b, half, 1) - b
        )
        return carry

    lax.fori_loop(0, total // chunk, piece, 0)


def gather(names, table, model_vis, column_gains):
    row_block, col_block, width = model_vis.shape
    pairs = row_block * col_block // 2
    total = names.shape[0]
    chunk = min(512, total)
    return pl.pallas_call(
        functools.partial(gather_kernel, col_block, chunk),
        out_shape=(
            jax.ShapeDtypeStruct((total, width), jnp.float32),
            jax.ShapeDtypeStruct((total,), jnp.int32),
        ),
        in_specs=[
            pl.BlockSpec(memory_space=pltpu.SMEM),
            pl.BlockSpec(memory_space=pltpu.SMEM),
            pl.BlockSpec(memory_space=pl.ANY),
            pl.BlockSpec(memory_space=pltpu.VMEM),
        ],
        out_specs=(
            pl.BlockSpec(memory_space=pltpu.VMEM),
            pl.BlockSpec(memory_space=pltpu.SMEM),
        ),
        scratch_shapes=[
            pltpu.VMEM((pairs, 2, width), jnp.bfloat16),
            pltpu.VMEM((2 * col_block, width), jnp.float32),
            pltpu.VMEM((2 * total, width), jnp.float32),
            pltpu.VMEM((2 * chunk, width), jnp.float32),
            pltpu.SemaphoreType.DMA,
        ],
        compiler_params=pltpu.CompilerParams(vmem_limit_bytes=56 << 20),
        cost_estimate=pl.CostEstimate(
            flops=1 << 20, bytes_accessed=model_vis.size * 2, transcendentals=0
        ),
        name="gather",
    )(names, table, model_vis.reshape(pairs, 2, width), column_gains)


def pick_rows(info, row_block, col_block):
    column_bits = col_block.bit_length()
    first = info >> (2 * column_bits + WEIGHT_BITS - 2)
    weight = ((info >> column_bits) & ((1 << WEIGHT_BITS) - 1)).astype(jnp.float32)
    spots = lax.broadcasted_iota(jnp.int32, (row_block, info.shape[1]), 0)
    return jnp.where(spots == first, weight, 0.0).astype(jnp.bfloat16)


def power_kernel(col_block, info_ref, c_ref, out_ref):
    row_block, width = out_ref.shape
    half = width // 2

    @pl.when(pl.program_id(0) == 0)
    def _():
        out_ref[...] = jnp.zeros_like(out_ref)

    c = c_ref[...]
    power = c * c
    power = power + pltpu.roll(power, half, 1)
    high = power.astype(jnp.bfloat16).astype(jnp.float32)
    low = lax.broadcasted_iota(jnp.int32, power.shape, 1) < half
    values = jnp.where(low, high, power - high).astype(jnp.bfloat16)
    sums = jnp.dot(
        pick_rows(info_ref[0], row_block, col_block), values, preferred_element_type=jnp.float32
    )
    out_ref[...] += sums + pltpu.roll(sums, half, 1)


def product_kernel(col_block, info_ref, c_ref, rows_ref, out_ref):
    row_block, width = out_ref.shape
    half = width // 2

    @pl.when(pl.program_id(0) == 0)
    def _():
        out_ref[...] = jnp.zeros_like(out_ref)

    c = c_ref[...]
    r = rows_ref[...].astype(jnp.float32)
    a = c * r
    b = c * pltpu.roll(r, half, 1)
    low = lax.broadcasted_iota(jnp.int32, c.shape, 1) < half
    product = jnp.where(low, a - pltpu.roll(a, half, 1), b + pltpu.roll(b, half, 1))
    high = product.astype(jnp.bfloat16)
    rest = (product - high.astype(jnp.float32)).astype(jnp.bfloat16)
    values = jnp.concatenate([high, rest], axis=1)
    sums = jnp.dot(
        pick_rows(info_ref[0], row_block, col_block), values, preferred_element_type=jnp.float32
    )
    out_ref[...] += sums[:, :width] + sums[:, width:]


def segment(kernel, name, info, arrays, row_block, col_block):
    total, width = arrays[0].shape
    chunk = min(1024, total)
    steps = total // chunk
    return pl.pallas_call(
        functools.partial(kernel, col_block),
        out_shape=jax.ShapeDtypeStruct((row_block, width), jnp.float32),
        grid=(steps,),
        in_specs=[pl.BlockSpec((1, 1, chunk), lambda i: (i, 0, 0))]
        + [pl.BlockSpec((chunk, width), lambda i: (i, 0))] * len(arrays),
        out_specs=pl.BlockSpec((row_block, width), lambda i: (0, 0)),
        cost_estimate=pl.CostEstimate(
            flops=2 * row_block * total * 2 * width,
            bytes_accessed=total * width * 4,
            transcendentals=0,
        ),
        name=name,
    )(info.reshape(steps, 1, chunk), *arrays)


def collect_kernel(
    count, num_ref, den_ref, out_ref, num_held, den_held, num_send, num_recv, den_send, den_recv
):
    me = lax.axis_index("acol")
    barrier = pltpu.get_barrier_semaphore()
    for step in range(1, count):
        pl.semaphore_signal(
            barrier,
            inc=1,
            device_id=(lax.axis_index("arow"), lax.rem(me + step, count)),
            device_id_type=MESH,
        )
    pl.semaphore_wait(barrier, count - 1)

    def copies(to, slot):
        return [
            pltpu.make_async_remote_copy(
                src_ref=part.at[to],
                dst_ref=held.at[slot],
                send_sem=send.at[to],
                recv_sem=recv.at[slot],
                device_id=(lax.axis_index("arow"), to),
                device_id_type=MESH,
            )
            for part, held, send, recv in (
                (den_ref, den_held, den_send, den_recv),
                (num_ref, num_held, num_send, num_recv),
            )
        ]

    for step in range(1, count):
        for copy in copies(lax.rem(me + step, count), me):
            copy.start()
    num = num_ref[me]
    den = den_ref[me]
    for step in range(1, count):
        other = lax.rem(me + step, count)
        for copy in copies(other, other):
            copy.wait()
        num = num + num_held[other]
        den = den + den_held[other]
    out_ref[...] = num / (den + RIDGE)


def collect(numerator, denominator, count):
    rows, width = numerator.shape
    share_rows = rows // count
    shape = (count, share_rows, width)
    return pl.pallas_call(
        functools.partial(collect_kernel, count),
        out_shape=jax.ShapeDtypeStruct((share_rows, width), jnp.float32),
        in_specs=[pl.BlockSpec(memory_space=pltpu.VMEM)] * 2,
        out_specs=pl.BlockSpec(memory_space=pltpu.VMEM),
        scratch_shapes=[pltpu.VMEM(shape, jnp.float32)] * 2
        + [pltpu.SemaphoreType.DMA((count,))] * 4,
        compiler_params=pltpu.CompilerParams(collective_id=1, has_side_effects=True),
        name="collect",
    )(numerator.reshape(shape), denominator.reshape(shape))


def split_parts(values, count):
    parts = []
    for _ in range(count - 1):
        high = values.astype(jnp.bfloat16)
        parts.append(high)
        values = values - high.astype(jnp.float32)
    parts.append(values.astype(jnp.bfloat16))
    return parts


def one_hot(found):
    return jnp.where(found, 1.0, 0.0).astype(jnp.bfloat16)


def contract(left, right, left_dim, right_dim):
    return lax.dot_general(
        left, right, (((left_dim,), (right_dim,)), ((), ())), preferred_element_type=jnp.float32
    )


def stream_kernel(
    row_count, col_count, near, lanes, chunk, fold,
    rows_ref, base_ref, gain_ref, pair_ref, weight_ref, model_ref,
    out_ref, flag_ref,
    model, rows_v, send_rows, send_labels, rank_ref, pos_ref, rows_in, name_in, label_v, label_s,
    table_v, table_s, first_ref, second_ref,
    column_ref, gain_parts, gain_rows, picked, c_table, c_rows, lookup, firsts, weights, sums,
    parts, half_in, halves, final_in,
    base_send, base_recv, name_send, name_recv, over_send, over_recv,
    half_send, half_recv, final_send, final_recv, gain_send, gain_recv, local_sem,
):
    devices = row_count * col_count
    count, width = rows_ref.shape
    half = width // 2
    blocks = count // LANES
    far = lanes - near
    table_rows = weight_ref.shape[0]
    slots = table_rows * LANES
    slot_bits = slots.bit_length() - 1
    row_block = sums.shape[0]
    col_block = gain_parts.shape[0]
    share_rows = gain_ref.shape[0]
    pairs = col_count // 2
    my_row = lax.axis_index("arow")
    my_col = lax.axis_index("acol")
    me = my_row * col_count + my_col
    parity = lax.rem(my_col, 2)
    my_pair = my_col // 2
    partner = my_col + 1 - 2 * parity
    aside = (my_row, partner)
    barrier = pltpu.get_barrier_semaphore()

    def place(index):
        return (index // col_count, lax.rem(index, col_count))

    def remote(src, dst, send, recv, to):
        return pltpu.make_async_remote_copy(
            src_ref=src, dst_ref=dst, send_sem=send, recv_sem=recv,
            device_id=to, device_id_type=MESH,
        )

    bring = pltpu.make_async_copy(rows_ref, rows_v, local_sem.at[1])
    bring.start()
    load = pltpu.make_async_copy(model_ref, model, local_sem.at[0])
    load.start()

    def greet(step, carry):
        pl.semaphore_signal(
            barrier, inc=1, device_id=place(lax.rem(me + step, devices)), device_id_type=MESH
        )
        return carry

    lax.fori_loop(1, devices, greet, 0)
    for line in range(table_rows):
        first_ref[line : line + 1, :] = jnp.clip(
            pair_ref[line, 0:1, :] - my_row * row_block, 0, row_block - 1
        )
        second_ref[line : line + 1, :] = jnp.clip(
            pair_ref[line, 1:2, :] - my_col * col_block, 0, col_block - 1
        )
    table_v[...] = first_ref[...] * (col_block // 2) + (second_ref[...] >> 1)

    upper = one_hot(
        lax.broadcasted_iota(jnp.int32, (LANES, LANES), 0)
        < lax.broadcasted_iota(jnp.int32, (LANES, LANES), 1)
    )
    tile = lax.broadcasted_iota(jnp.int32, (devices, LANES), 0)
    before = jnp.zeros((devices, 1), jnp.float32)
    for block in range(blocks):
        hit = tile == base_ref[block : block + 1, :] >> slot_bits
        hits = jnp.where(hit, 1.0, 0.0)
        within = jnp.dot(hits.astype(jnp.bfloat16), upper, preferred_element_type=jnp.float32)
        ranking = jnp.sum(jnp.where(hit, within + before, 0.0), axis=0, keepdims=True)
        before = before + jnp.sum(hits, axis=1, keepdims=True)
        rank_ref[block : block + 1, :] = ranking.astype(jnp.int32)
    ranks = rank_ref[...]
    over = ranks >= near
    overs = one_hot(over)
    lower = one_hot(
        lax.broadcasted_iota(jnp.int32, (blocks, blocks), 0)
        > lax.broadcasted_iota(jnp.int32, (blocks, blocks), 1)
    )
    earlier = jnp.dot(lower, overs, preferred_element_type=jnp.float32)
    over_rank = jnp.dot(overs, upper, preferred_element_type=jnp.float32) + jnp.sum(
        earlier, axis=1, keepdims=True
    )
    over_spot = near + over_rank.astype(jnp.int32)
    lost = jnp.max(jnp.where(over & (over_spot >= lanes), 1.0, 0.0), axis=(0, 1), keepdims=True)
    over_at = jnp.where(over, over_spot, -1)
    pos_ref[...] = jnp.where(
        over,
        jnp.where(over_spot < lanes, devices * near + over_spot - near, -1),
        (base_ref[...] >> slot_bits) * near + ranks,
    )

    spots = lax.broadcasted_iota(jnp.int32, (LANES, LANES), 0)
    over_spots = lax.broadcasted_iota(jnp.int32, (lanes, LANES), 0)
    sub = lax.broadcasted_iota(jnp.int32, (8, LANES), 0)
    names = jnp.zeros((3 * devices, LANES), jnp.float32)
    marks = jnp.zeros((8, lanes), jnp.float32)
    for block in range(blocks):
        slot = base_ref[block : block + 1, :]
        owner = slot >> slot_bits
        high = ((slot & (slots - 1)) >> 6).astype(jnp.float32)
        low_bits = (slot & 63).astype(jnp.float32)
        hit = tile == owner
        pieces = jnp.concatenate(
            [jnp.where(hit, high, 0.0), jnp.where(hit, low_bits, 0.0), jnp.where(hit, 1.0, 0.0)],
            axis=0,
        ).astype(jnp.bfloat16)
        names = names + contract(pieces, one_hot(spots == ranks[block : block + 1, :]), 1, 1)
        whole = jnp.where(
            sub == 0,
            owner.astype(jnp.float32),
            jnp.where(sub == 1, high, jnp.where(sub == 2, low_bits, jnp.where(sub == 3, 1.0, 0.0))),
        ).astype(jnp.bfloat16)
        marks = marks + contract(
            whole, one_hot(over_spots == over_at[block : block + 1, :]), 1, 1
        )
    lane = lax.broadcasted_iota(jnp.int32, (devices, LANES), 1)
    label = names[:devices] * 64.0 + names[devices : 2 * devices]
    label = jnp.where(names[2 * devices :] > 0.5, label, float(slots))
    label = jnp.where(lane == LANES - 1, lost, label).astype(jnp.int32)
    mark = marks[0:1] * float(slots) + marks[1:2] * 64.0 + marks[2:3]
    mark = jnp.where(marks[3:4] > 0.5, mark, -1.0).astype(jnp.int32)
    for index in range(devices):
        send_labels[index] = jnp.concatenate([label[index : index + 1, :], mark], axis=1)
    name_in[me] = send_labels[me]

    pl.semaphore_wait(barrier, devices - 1)

    def name_copy(to, slot):
        return remote(
            send_labels.at[to], name_in.at[slot], name_send, name_recv, place(to)
        )

    def base_copy(to, slot):
        return remote(
            send_rows.at[to], rows_in.at[slot, pl.ds(0, near)],
            base_send, base_recv.at[my_row], place(to),
        )

    def over_copy(sources, to, stage):
        there = rows_in.at[sources, pl.ds(near, far)]
        return remote(there, there, over_send, over_recv.at[stage], to)

    def along(step):
        return over_copy(me, (lax.rem(my_row + step, row_count), my_col), 0)

    def across(source_row, step):
        to = (my_row, lax.rem(my_col + 2 * step, col_count))
        return over_copy(source_row * col_count + my_col, to, 1)

    def relay(source):
        return over_copy(source, (my_row, partner), 2)

    column = me // row_count
    part = lax.rem(me, row_count)

    def gain_copy(row, col, slot):
        return remote(
            gain_ref, column_ref.at[slot], gain_send.at[row], gain_recv.at[slot], (row, col)
        )

    for row in range(row_count):
        stays = jnp.logical_and(row == my_row, column == my_col)

        @pl.when(jnp.logical_not(stays))
        def _():
            gain_copy(row, column, part).start()

        @pl.when(stays)
        def _():
            column_ref[part] = gain_ref[...]

    def send_names(step, carry):
        name_copy(lax.rem(me + step, devices), me).start()
        return carry

    lax.fori_loop(1, devices, send_names, 0)

    def arrange(first, size):
        at = lax.broadcasted_iota(jnp.int32, (size, LANES), 0) + first
        hot = jnp.concatenate(
            [one_hot(at == pos_ref[block : block + 1, :]) for block in range(blocks)], axis=1
        )
        return jnp.dot(hot, rows_v[...], preferred_element_type=jnp.float32).astype(jnp.bfloat16)

    bring.wait()
    rows_in[me, near:, :] = arrange(devices * near, far)
    for step in range(1, row_count):
        along(step).start()
    for step in range(1, pairs):
        across(my_row, step).start()
    relay(me).start()


    groups = devices // fold

    def arrange_tiles(step, carry):
        group = lax.rem(step + (my_row + 1) * (col_count // fold), groups)
        got = arrange(group * (fold * near), fold * near)
        send_rows[pl.ds(group * fold, fold)] = got.reshape(fold, near, width)

        @pl.when(step < groups - col_count // fold)
        def _():
            for number in range(fold):
                base_copy(group * fold + number, me).start()

        return carry

    lax.fori_loop(0, groups, arrange_tiles, 0)
    rows_in[me, :near, :] = send_rows[me]

    def send_plane(step, carry):
        base_copy(my_row * col_count + lax.rem(my_col + step, col_count), me).start()
        return carry

    lax.fori_loop(1, col_count, send_plane, 0)

    for slot in range(row_count):
        source = my_col * row_count + slot

        @pl.when(source != me)
        def _():
            gain_copy(0, my_col, slot).wait_recv()

    gains = split_parts(column_ref[...].reshape(col_block, width), 3)
    for number in range(3):
        gain_parts[:, number * width : (number + 1) * width] = gains[number]
    gain_parts[:, 3 * width :] = one_hot(
        (lax.broadcasted_iota(jnp.int32, (col_block, width), 0) & 1) == 1
    )
    seconds = lax.broadcasted_iota(jnp.int32, (col_block, LANES), 0)

    def spread_gains(number, carry):
        hot = jnp.concatenate(
            [
                one_hot(seconds == second_ref[pl.ds(number * (chunk // LANES) + k, 1), :])
                for k in range(chunk // LANES)
            ],
            axis=1,
        )
        got = contract(hot, gain_parts[...], 0, 0)
        at = pl.ds(pl.multiple_of(number * chunk, chunk), chunk)
        gain_rows[at, :width] = (got[:, :width] + got[:, width : 2 * width]) + got[
            :, 2 * width : 3 * width
        ]
        gain_rows[at, width:] = got[:, 3 * width :]
        return carry

    lax.fori_loop(0, slots // chunk, spread_gains, 0)
    to_table = pltpu.make_async_copy(table_v, table_s, local_sem.at[2])
    to_table.start()
    to_table.wait()
    lookup[:table_rows, :] = (first_ref[...] >> 1).astype(jnp.float32).astype(jnp.bfloat16)
    lookup[table_rows:, :] = (
        (((first_ref[...] & 1) << WEIGHT_BITS) + weight_ref[...]).astype(jnp.float32)
    ).astype(jnp.bfloat16)

    remote(
        send_labels.at[pl.ds(0, devices - 1)], name_in.at[pl.ds(0, devices - 1)],
        name_send, name_recv, aside,
    ).wait()
    lane = lax.broadcasted_iota(jnp.int32, name_in.shape, 2)
    flag_ref[0, 0] = jnp.max(jnp.where(lane == LANES - 1, name_in[...], 0).astype(jnp.float32)).astype(
        jnp.int32
    )
    lane = lax.broadcasted_iota(jnp.int32, (1, LANES), 1)
    batch = fold * lanes

    def name_rows(step, carry):
        labels = []
        for number in range(fold):
            source = step * fold + number
            there = name_in[source][:, LANES:] - me * slots
            there = jnp.where((there >= 0) & (there < slots), there, slots)
            near_part = jnp.where(lane < near, name_in[source][:, :LANES], there[:, :LANES])
            if lanes > LANES:
                near_part = jnp.concatenate([near_part, there[:, LANES:]], axis=1)
            near_part = jnp.clip(near_part, 0, slots)
            for line in range(lanes // LANES):
                label_v[source * (lanes // LANES) + line] = near_part[
                    :, line * LANES : (line + 1) * LANES
                ]
            labels.append(near_part)
        label = jnp.concatenate(labels, axis=1)
        hot = one_hot(lax.broadcasted_iota(jnp.int32, (LANES, batch), 0) == (label & (LANES - 1)))
        found = jnp.dot(lookup[...], hot, preferred_element_type=jnp.float32)
        line = lax.broadcasted_iota(jnp.int32, (table_rows, batch), 0) == label >> 7
        upper_bits = jnp.sum(
            jnp.where(line, found[:table_rows], 0.0), axis=0, keepdims=True
        ).astype(jnp.int32)
        rest = jnp.sum(
            jnp.where(line, found[table_rows:], 0.0), axis=0, keepdims=True
        ).astype(jnp.int32)
        firsts[step] = 2 * upper_bits + (rest >> WEIGHT_BITS)
        weights[step] = (rest & ((1 << WEIGHT_BITS) - 1)).astype(jnp.float32)
        return carry

    lax.fori_loop(0, devices // fold, name_rows, 0)
    to_scalar = pltpu.make_async_copy(label_v, label_s, local_sem.at[1])
    to_scalar.start()

    over_copy(pl.ds(0, row_count - 1), aside, 0).wait_recv()
    for step in range(1, row_count):
        source_row = lax.rem(my_row + step, row_count)
        for other in range(1, pairs):
            across(source_row, other).start()
        relay(source_row * col_count + my_col).start()

    load.wait()
    low = lax.broadcasted_iota(jnp.int32, (chunk, width), 1) < half
    c_table[slots:, :] = jnp.zeros((c_table.shape[0] - slots, width), jnp.float32)

    def piece(number, carry):
        begin = number * chunk

        def fetch(line, carry):
            to = pl.multiple_of(line * 2 * LANES, 2 * LANES)
            window = table_s.at[number * (chunk // LANES) + line]
            for at in range(0, LANES, GROUP):
                held = [model[window[at + k]].astype(jnp.float32) for k in range(GROUP)]
                for k in range(GROUP):
                    picked[pl.ds(to + 2 * (at + k), 2), :] = held[k]
            return carry

        lax.fori_loop(0, chunk // LANES, fetch, 0)
        at = pl.ds(pl.multiple_of(begin, chunk), chunk)
        m = jnp.where(
            gain_rows[at, width:] > 0.5,
            picked[pl.ds(1, chunk, stride=2), :],
            picked[pl.ds(0, chunk, stride=2), :],
        )
        g = gain_rows[at, :width]
        a = m * g
        b = m * pltpu.roll(g, half, 1)
        c_table[at, :] = jnp.where(
            low, a + pltpu.roll(a, half, 1), pltpu.roll(b, half, 1) - b
        )
        return carry

    lax.fori_loop(0, slots // chunk, piece, 0)

    to_scalar.wait()

    def grab(line, carry):
        to = pl.multiple_of(line * LANES, LANES)
        window = label_s.at[line, 0]
        for at in range(0, LANES, GROUP):
            held = [c_table[pl.ds(window[at + k], 1), :] for k in range(GROUP)]
            for k in range(GROUP):
                c_rows[pl.ds(to + at + k, 1), :] = held[k]
        return carry

    middle = devices * lanes // LANES // 2
    lax.fori_loop(0, middle, grab, 0)
    over_copy(pl.ds(0, row_count * (pairs - 1)), aside, 1).wait_recv()
    for step in range(1, pairs):
        for source_row in range(row_count):
            source = source_row * col_count + lax.rem(my_col + 2 * step, col_count)
            over_copy(source, aside, 2).start()

    lax.fori_loop(middle, 2 * middle, grab, 0)
    low = lax.broadcasted_iota(jnp.int32, (batch, width), 1) < half
    sums[...] = jnp.zeros_like(sums)

    over_copy(pl.ds(0, row_count * pairs), aside, 2).wait_recv()

    def plane_arrived(row, count):
        remote(
            send_rows.at[pl.ds(0, count)], rows_in.at[pl.ds(0, count), pl.ds(0, near)],
            base_send, base_recv.at[row], aside,
        ).wait_recv()

    def add_product(step, carry):
        c = c_rows[pl.ds(pl.multiple_of(step * batch, batch), batch), :]
        r = rows_in[pl.ds(step * fold, fold)].reshape(batch, width).astype(jnp.float32)
        turned = pltpu.roll(c, half, 1)
        product = jnp.where(low, c, turned) * r + jnp.where(low, -turned, c) * pltpu.roll(
            r, half, 1
        )
        power = c * c
        power = power + pltpu.roll(power, half, 1)
        power_high = power.astype(jnp.bfloat16).astype(jnp.float32)
        power = jnp.where(low, power_high, power - power_high).astype(jnp.bfloat16)
        values = jnp.concatenate(split_parts(product, 2) + [power], axis=1)
        pick = jnp.where(
            lax.broadcasted_iota(jnp.int32, (row_block, batch), 0) == firsts[step],
            weights[step],
            0.0,
        ).astype(jnp.bfloat16)
        sums[...] += jnp.dot(pick, values, preferred_element_type=jnp.float32)
        return carry

    steps = col_count // fold
    upper_half = my_row // (row_count // 2)

    def add_plane(turn, carry):
        rising = turn - 1 + (turn - 1 - my_row + row_count) // row_count
        falling = row_count - turn - (my_row + turn) // row_count
        other = (1 - upper_half) * rising + upper_half * falling
        plane_arrived(other, col_count)
        return lax.fori_loop(0, steps, lambda step, held: add_product(other * steps + step, held), carry)

    plane_arrived(my_row, col_count - 1)
    lax.fori_loop(0, steps, lambda step, held: add_product(my_row * steps + step, held), 0)
    lax.fori_loop(1, row_count, add_plane, 0)
    remote(
        send_rows.at[pl.ds(0, devices - 1)], rows_in.at[pl.ds(0, devices - 1), pl.ds(0, near)],
        base_send, base_recv.at[0], aside,
    ).wait_send()

    numerator = sums[:, :width] + sums[:, width : 2 * width]
    denominator = sums[:, 2 * width :]
    denominator = denominator + pltpu.roll(denominator, half, 1)
    side = share_rows // 2
    low = lax.broadcasted_iota(jnp.int32, (side, width), 1) < half
    for col in range(col_count):
        at = col * share_rows
        parts[col % 2, col // 2, :share_rows, :] = numerator[at : at + share_rows]
        parts[col % 2, col // 2, share_rows:, :] = jnp.where(
            low, denominator[at : at + side], denominator[at + side : at + share_rows]
        )
    swap = remote(
        parts.at[1 - parity], half_in, half_send, half_recv, (my_row, partner)
    )
    swap.start()

    over_copy(pl.ds(0, devices - 1), aside, 0).wait_send()
    for row in range(row_count):
        stays = jnp.logical_and(row == my_row, column == my_col)

        @pl.when(jnp.logical_not(stays))
        def _():
            gain_copy(row, column, part).wait_send()

    swap.wait()
    halves[...] = parts[parity] + half_in[...]

    def final_copy(to, slot, device):
        return remote(halves.at[to], final_in.at[slot], final_send, final_recv, device)

    for step in range(1, pairs):
        to = lax.rem(my_pair + step, pairs)
        final_copy(to, my_pair, (my_row, 2 * to + parity)).start()
    final_copy(pl.ds(0, pairs - 1), pl.ds(0, pairs - 1), aside).wait()
    total = halves[my_pair]
    for step in range(1, pairs):
        total = total + final_in[lax.rem(my_pair + step, pairs)]
    held = total[share_rows:]
    turned = pltpu.roll(held, half, 1)
    out_ref[:side, :] = total[:side] / (jnp.where(low, held, turned) + RIDGE)
    out_ref[side:, :] = total[side:share_rows] / (jnp.where(low, turned, held) + RIDGE)


def stream(rows, baseline, gains, pair_table, weight, model_vis, row_count, col_count):
    devices = row_count * col_count
    count, width = rows.shape
    row_block, col_block, _ = model_vis.shape
    slots = weight.shape[0]
    share_rows = gains.shape[0]
    mean = count // devices
    capacity = 4 * mean
    lanes = -(-capacity // LANES) * LANES
    near = -(-11 * mean // 64) * 8
    far = lanes - near
    blocks = count // LANES
    pairs = row_block * col_block // 2
    total = devices * lanes
    chunk = min(512, slots)
    fold = 4
    half_count = col_count // 2
    piece = (half_count, share_rows + share_rows // 2, width)
    vmem = pl.BlockSpec(memory_space=pltpu.VMEM)
    dma = pltpu.SemaphoreType.DMA
    return pl.pallas_call(
        functools.partial(stream_kernel, row_count, col_count, near, lanes, chunk, fold),
        out_shape=(
            jax.ShapeDtypeStruct(gains.shape, jnp.float32),
            jax.ShapeDtypeStruct((1, 1), jnp.int32),
        ),
        in_specs=[pl.BlockSpec(memory_space=pl.ANY)]
        + [vmem] * 4
        + [pl.BlockSpec(memory_space=pl.ANY)],
        out_specs=(vmem, pl.BlockSpec(memory_space=pltpu.SMEM)),
        scratch_shapes=[
            pltpu.VMEM((pairs, 2, width), jnp.bfloat16),
            pltpu.VMEM((count, width), jnp.bfloat16),
            pltpu.VMEM((devices, near, width), jnp.bfloat16),
            pltpu.VMEM((devices, 1, LANES + lanes), jnp.int32),
            pltpu.VMEM((blocks, LANES), jnp.int32),
            pltpu.VMEM((blocks, LANES), jnp.int32),
            pltpu.VMEM((devices, lanes, width), jnp.bfloat16),
            pltpu.VMEM((devices, 1, LANES + lanes), jnp.int32),
            pltpu.VMEM((total // LANES, 1, LANES), jnp.int32),
            pltpu.SMEM((total // LANES, 1, LANES), jnp.int32),
            pltpu.VMEM((slots // LANES, LANES), jnp.int32),
            pltpu.SMEM((slots // LANES, LANES), jnp.int32),
            pltpu.VMEM((slots // LANES, LANES), jnp.int32),
            pltpu.VMEM((slots // LANES, LANES), jnp.int32),
            pltpu.VMEM((row_count, share_rows, width), jnp.float32),
            pltpu.VMEM((col_block, 4 * width), jnp.bfloat16),
            pltpu.VMEM((slots, 2 * width), jnp.float32),
            pltpu.VMEM((2 * chunk, width), jnp.float32),
            pltpu.VMEM((slots + 8, width), jnp.float32),
            pltpu.VMEM((total, width), jnp.float32),
            pltpu.VMEM((2 * slots // LANES, LANES), jnp.bfloat16),
            pltpu.VMEM((devices // fold, 1, fold * lanes), jnp.int32),
            pltpu.VMEM((devices // fold, 1, fold * lanes), jnp.float32),
            pltpu.VMEM((row_block, 3 * width), jnp.float32),
            pltpu.VMEM((2,) + piece, jnp.float32),
            pltpu.VMEM(piece, jnp.float32),
            pltpu.VMEM(piece, jnp.float32),
            pltpu.VMEM(piece, jnp.float32),
        ]
        + [dma]
        + [dma((row_count,))]
        + [dma] * 3
        + [dma((3,))]
        + [dma] * 4
        + [dma((row_count,))] * 2
        + [dma((3,))],
        compiler_params=pltpu.CompilerParams(
            collective_id=2, has_side_effects=True, vmem_limit_bytes=63 << 20
        ),
        name="stream",
    )(
        rows,
        baseline.reshape(blocks, LANES),
        gains,
        pair_table.reshape(slots // LANES, LANES, 2).transpose(0, 2, 1),
        weight.reshape(slots // LANES, LANES),
        model_vis.reshape(pairs, 2, width),
    )


def padded(row_count, col_count, row_data, row_baseline, pair_table, lengths, model_vis, gains):
    devices = row_count * col_count
    slots = lengths.shape[0]
    capacity = 4 * row_data.shape[0] // devices
    row_block, col_block, width = model_vis.shape
    total = devices * capacity
    my_row = lax.axis_index("arow")
    my_col = lax.axis_index("acol")
    first = pair_table[:, 0] - my_row * row_block
    second = pair_table[:, 1] - my_col * col_block
    pair = first * (col_block // 2) + second // 2
    table = ((pair << WEIGHT_BITS) + lengths) * (2 * col_block) + 2 * second
    table = jnp.concatenate([table, jnp.zeros((LANES,), jnp.int32)])
    outgoing, labels = route(row_data, row_baseline, devices, capacity, slots)
    names, column_gains = share(
        labels.reshape(devices, 1, capacity), gains, row_count, col_count
    )
    outgoing, names = lax.optimization_barrier((outgoing, names))
    arrived = lax.all_to_all(
        outgoing.reshape(devices, capacity, width),
        ("arow", "acol"),
        split_axis=0,
        concat_axis=0,
        tiled=True,
    ).reshape(total, width)
    c, info = gather(
        names.reshape(total), table, model_vis, column_gains.reshape(col_block, width)
    )
    power = segment(power_kernel, "power", info, [c], row_block, col_block)
    product = segment(product_kernel, "product", info, [c, arrived], row_block, col_block)
    return collect(product, power, col_count)


def local(row_count, col_count, row_data, row_baseline, pair_table, lengths, model_vis, gains):
    updated, flag = stream(
        row_data, row_baseline, gains, pair_table, lengths, model_vis, row_count, col_count
    )
    return lax.cond(
        flag[0, 0] > 0,
        lambda: padded(
            row_count, col_count, row_data, row_baseline, pair_table, lengths, model_vis, gains
        ),
        lambda: updated,
    )


def solution(mesh):
    placed = (
        P(("arow", "acol"), None),
        P(("arow", "acol")),
        P(("arow", "acol"), None),
        P(("arow", "acol")),
        P("arow", "acol", None),
        P(("arow", "acol"), None),
    )
    return jax.shard_map(
        functools.partial(local, mesh.shape["arow"], mesh.shape["acol"]),
        mesh=mesh,
        in_specs=placed,
        out_specs=P(("arow", "acol"), None),
        check_vma=False,
    )
```
